16 devices in a mesh: fsdp: 16 (over z, y, x, core).
Axes of the slice: x: 2, y: 2, z: 2, core: 2. Of those that a mesh axis runs over, the one named last changes fastest.
Arguments:
- x: bfloat16 [32, 1024, 1024], P('fsdp')
- lengths: int32 [32], P('fsdp')
- d_y: bfloat16 [32, 1024, 1024], P('fsdp')
- w_attn: bfloat16 [2, 4, 1024, 1024], P(None, None, 'fsdp')
- b_attn: bfloat16 [2, 4, 1024], P(None, None, 'fsdp')
- ln_par: bfloat16 [2, 4, 1024], P(None, None, 'fsdp')
- w_up: bfloat16 [2, 1024, 4096], P(None, 'fsdp')
- b_up: bfloat16 [2, 4096], P(None, 'fsdp')
- w_down: bfloat16 [2, 4096, 1024], P(None, 'fsdp')
- b_down: bfloat16 [2, 1024], P(None, 'fsdp')
Outputs:
- output 1: bfloat16 [32, 1024, 1024], P('fsdp')
- output 2: float32 [2, 4, 1024, 1024], P(None, None, 'fsdp')
- output 3: float32 [2, 4, 1024], P(None, None, 'fsdp')
- output 4: float32 [2, 4, 1024], P(None, None, 'fsdp')
- output 5: float32 [2, 1024, 4096], P(None, 'fsdp')
- output 6: float32 [2, 4096], P(None, 'fsdp')
- output 7: float32 [2, 4096, 1024], P(None, 'fsdp')
- output 8: float32 [2, 1024], P(None, 'fsdp')
All inputs are finite; a program needn't handle non-finite values.
Results may differ from the reference program's by a relative error of at most 0.013046.
Values are sent between devices in bfloat16 or wider.
A program may use at most 1 GiB of HBM per device.

```python
import jax
import jax.numpy as jnp
from jax import lax

MODEL_DIM = 1024
FFN_DIM = 4096
HEAD_DIM = 64
NUM_LAYERS = 2
SEQ_LEN = 1024
SEQ_DEV = 2
GROUP_SIZE = 16
EPS = 1e-5
THETA = 10000.0
NUM_HEADS = MODEL_DIM // HEAD_DIM
BATCH = SEQ_DEV * GROUP_SIZE
MIN_LEN = SEQ_LEN // 8


def setup_inputs(seed: int = 0) -> dict:
    key_list = jax.random.split(jax.random.key(seed), 10)
    seq_index = jnp.arange(BATCH)
    drawn_len = jax.random.randint(key_list[1], (BATCH,), MIN_LEN, SEQ_LEN + 1)
    lengths = jnp.where(seq_index == 0, SEQ_LEN, jnp.where(seq_index == 1, MIN_LEN, drawn_len)).astype(jnp.int32)
    act_shape = (BATCH, SEQ_LEN, MODEL_DIM)
    dy_scale = float(BATCH * SEQ_LEN) ** -0.25
    ln_base = jnp.array([1.0, 0.0, 1.0, 0.0], dtype=jnp.float32)[None, :, None]
    return {
        'x': jax.random.normal(key_list[0], act_shape, jnp.float32).astype(jnp.bfloat16),
        'lengths': lengths,
        'd_y': (dy_scale * jax.random.normal(key_list[2], act_shape, jnp.float32)).astype(jnp.bfloat16),
        'w_attn': (MODEL_DIM ** -0.5 * jax.random.normal(key_list[3], (NUM_LAYERS, 4, MODEL_DIM, MODEL_DIM), jnp.float32)).astype(jnp.bfloat16),
        'b_attn': (0.3 * jax.random.normal(key_list[4], (NUM_LAYERS, 4, MODEL_DIM), jnp.float32)).astype(jnp.bfloat16),
        'ln_par': (ln_base + 0.2 * jax.random.normal(key_list[5], (NUM_LAYERS, 4, MODEL_DIM), jnp.float32)).astype(jnp.bfloat16),
        'w_up': (MODEL_DIM ** -0.5 * jax.random.normal(key_list[6], (NUM_LAYERS, MODEL_DIM, FFN_DIM), jnp.float32)).astype(jnp.bfloat16),
        'b_up': (0.5 * jax.random.normal(key_list[7], (NUM_LAYERS, FFN_DIM), jnp.float32)).astype(jnp.bfloat16),
        'w_down': (FFN_DIM ** -0.5 * jax.random.normal(key_list[8], (NUM_LAYERS, FFN_DIM, MODEL_DIM), jnp.float32)).astype(jnp.bfloat16),
        'b_down': (0.3 * jax.random.normal(key_list[9], (NUM_LAYERS, MODEL_DIM), jnp.float32)).astype(jnp.bfloat16),
    }


def to_bf16(tensor):
    return tensor.astype(jnp.bfloat16).astype(jnp.float32)


def norm_fwd(x_in, gain, shift):
    row_mean = jnp.mean(x_in, axis=-1, keepdims=True)
    centered = x_in - row_mean
    variance = jnp.mean(centered * centered, axis=-1, keepdims=True)
    return centered * lax.rsqrt(variance + EPS) * gain + shift


def rotary_tables():
    half_dim = HEAD_DIM // 2
    inv_freq = 1.0 / (THETA ** (jnp.arange(half_dim, dtype=jnp.float32) * (2.0 / HEAD_DIM)))
    angles = jnp.arange(SEQ_LEN, dtype=jnp.float32)[:, None] * inv_freq[None, :]
    return jnp.cos(angles)[:, None, :], jnp.sin(angles)[:, None, :]


def rotate(tensor, cos_tab, sin_tab):
    half_dim = HEAD_DIM // 2
    first_half = tensor[..., :half_dim]
    second_half = tensor[..., half_dim:]
    return jnp.concatenate([first_half * cos_tab - second_half * sin_tab, second_half * cos_tab + first_half * sin_tab], axis=-1)


def layer_fwd(x, weights, lengths, tables):
    w_attn, b_attn, ln_par, w_up, b_up, w_down, b_down = weights
    cos_tab, sin_tab = tables
    num_seq = x.shape[0]
    h_one = to_bf16(norm_fwd(x, ln_par[0], ln_par[1]))
    projected = jnp.einsum('bld,kde->kble', h_one, w_attn[:3]) + b_attn[:3, None, None, :]
    projected = projected.reshape(3, num_seq, SEQ_LEN, NUM_HEADS, HEAD_DIM)
    query_rot = to_bf16(rotate(projected[0] * (HEAD_DIM ** -0.5), cos_tab, sin_tab))
    key_rot = to_bf16(rotate(projected[1], cos_tab, sin_tab))
    values = to_bf16(projected[2])
    scores = jnp.einsum('bqhd,bkhd->bhqk', query_rot, key_rot)
    key_valid = jnp.arange(SEQ_LEN)[None, None, None, :] < lengths[:, None, None, None]
    attn_probs = to_bf16(jax.nn.softmax(jnp.where(key_valid, scores, -1e30), axis=-1))
    context = to_bf16(jnp.einsum('bhqk,bkhd->bqhd', attn_probs, values)).reshape(num_seq, SEQ_LEN, MODEL_DIM)
    x_mid = to_bf16(x + jnp.einsum('bld,de->ble', context, w_attn[3]) + b_attn[3])
    h_two = to_bf16(norm_fwd(x_mid, ln_par[2], ln_par[3]))
    act_out = to_bf16(jax.nn.gelu(jnp.einsum('bld,df->blf', h_two, w_up) + b_up, approximate=False))
    return to_bf16(x_mid + jnp.einsum('blf,fd->bld', act_out, w_down) + b_down)


def reference(x, lengths, d_y, w_attn, b_attn, ln_par, w_up, b_up, w_down, b_down):
    params = tuple(tensor.astype(jnp.float32) for tensor in (w_attn, b_attn, ln_par, w_up, b_up, w_down, b_down))
    tables = rotary_tables()

    def stack_fwd(x_block, param_set, len_block):
        hidden = x_block
        for layer_idx in range(NUM_LAYERS):
            hidden = layer_fwd(hidden, tuple(tensor[layer_idx] for tensor in param_set), len_block, tables)
        return hidden

    def block_step(grad_acc, block_in):
        x_block, len_block, dy_block = block_in

        def block_fwd(x_local, param_local):
            return stack_fwd(x_local, param_local, len_block)

        _, pull_back = jax.vjp(block_fwd, x_block.astype(jnp.float32), params)
        d_x_block, d_params = pull_back(dy_block.astype(jnp.float32))
        return jax.tree.map(jnp.add, grad_acc, d_params), d_x_block.astype(jnp.bfloat16)

    grad_zero = jax.tree.map(jnp.zeros_like, params)
    blocks_in = (x.reshape(GROUP_SIZE, SEQ_DEV, SEQ_LEN, MODEL_DIM), lengths.reshape(GROUP_SIZE, SEQ_DEV), d_y.reshape(GROUP_SIZE, SEQ_DEV, SEQ_LEN, MODEL_DIM))
    grad_sum, d_x = lax.scan(block_step, grad_zero, blocks_in)
    return (d_x.reshape(BATCH, SEQ_LEN, MODEL_DIM), grad_sum[0], grad_sum[1], grad_sum[2], grad_sum[3], grad_sum[4], grad_sum[5], grad_sum[6])
```

```python
import math
import functools
import jax
import jax.numpy as jnp
from jax import lax
from jax.sharding import PartitionSpec as P

HEAD_DIM = 64
EPS = 1e-5
THETA = 10000.0
NEG_BIG = -1e30


def rotary_tables(seq_len):
    half_dim = HEAD_DIM // 2
    inv_freq = 1.0 / (THETA ** (jnp.arange(half_dim, dtype=jnp.float32) * (2.0 / HEAD_DIM)))
    angles = jnp.arange(seq_len, dtype=jnp.float32)[:, None] * inv_freq[None, :]
    return jnp.cos(angles)[:, None, :], jnp.sin(angles)[:, None, :]


def rotate(tensor, cos_tab, sin_tab):
    half_dim = HEAD_DIM // 2
    first_half = tensor[..., :half_dim]
    second_half = tensor[..., half_dim:]
    return jnp.concatenate([first_half * cos_tab - second_half * sin_tab, second_half * cos_tab + first_half * sin_tab], axis=-1)


def rotate_back(tensor, cos_tab, sin_tab):
    half_dim = HEAD_DIM // 2
    first_half = tensor[..., :half_dim]
    second_half = tensor[..., half_dim:]
    return jnp.concatenate([first_half * cos_tab + second_half * sin_tab, second_half * cos_tab - first_half * sin_tab], axis=-1)


def norm_fwd(x_in, gain, shift):
    row_mean = jnp.mean(x_in, axis=-1, keepdims=True)
    centered = x_in - row_mean
    variance = jnp.mean(centered * centered, axis=-1, keepdims=True)
    return centered * lax.rsqrt(variance + EPS) * gain + shift


def gelu_slope(pre_act):
    normal_cdf = 0.5 * (1.0 + lax.erf(pre_act * (1.0 / math.sqrt(2.0))))
    density = jnp.exp(-0.5 * pre_act * pre_act) * (1.0 / math.sqrt(2.0 * math.pi))
    return normal_cdf + pre_act * density


def layer_forward(x, weights, lengths, tables):
    w_attn, b_attn, ln_par, w_up, b_up, w_down, b_down = weights
    cos_tab, sin_tab = tables
    num_seq, seq_len, model_dim = x.shape
    num_heads = model_dim // HEAD_DIM
    x_f32 = x.astype(jnp.float32)
    h_one = norm_fwd(x_f32, ln_par[0].astype(jnp.float32), ln_par[1].astype(jnp.float32)).astype(jnp.bfloat16)
    projected = jnp.einsum('bld,kde->kble', h_one, w_attn[:3], preferred_element_type=jnp.float32)
    projected = (projected + b_attn[:3, None, None, :].astype(jnp.float32)).reshape(3, num_seq, seq_len, num_heads, HEAD_DIM)
    query_rot = rotate(projected[0] * (HEAD_DIM ** -0.5), cos_tab, sin_tab).astype(jnp.bfloat16)
    key_rot = rotate(projected[1], cos_tab, sin_tab).astype(jnp.bfloat16)
    values = projected[2].astype(jnp.bfloat16)
    scores = jnp.einsum('bqhd,bkhd->bhqk', query_rot, key_rot, preferred_element_type=jnp.float32)
    key_valid = jnp.arange(seq_len)[None, None, None, :] < lengths[:, None, None, None]
    probs_bf = jax.nn.softmax(jnp.where(key_valid, scores, NEG_BIG), axis=-1).astype(jnp.bfloat16)
    context = jnp.einsum('bhqk,bkhd->bqhd', probs_bf, values, preferred_element_type=jnp.float32)
    context = context.astype(jnp.bfloat16).reshape(num_seq, seq_len, model_dim)
    attn_out = jnp.einsum('bld,de->ble', context, w_attn[3], preferred_element_type=jnp.float32)
    x_mid = (x_f32 + attn_out + b_attn[3].astype(jnp.float32)).astype(jnp.bfloat16)
    mid_f32 = x_mid.astype(jnp.float32)
    h_two = norm_fwd(mid_f32, ln_par[2].astype(jnp.float32), ln_par[3].astype(jnp.float32)).astype(jnp.bfloat16)
    pre_act = jnp.einsum('bld,df->blf', h_two, w_up, preferred_element_type=jnp.float32) + b_up.astype(jnp.float32)
    act_bf = jax.nn.gelu(pre_act, approximate=False).astype(jnp.bfloat16)
    mlp_out = jnp.einsum('blf,fd->bld', act_bf, w_down, preferred_element_type=jnp.float32)
    y_out = (mid_f32 + mlp_out + b_down.astype(jnp.float32)).astype(jnp.bfloat16)
    saved_acts = (x, h_one, query_rot, key_rot, values, probs_bf, context, x_mid, h_two, pre_act, act_bf)
    return y_out, saved_acts


def layer_backward(d_out, saved_acts, weights, tables):
    w_attn, ln_par, w_up, w_down = weights[0], weights[2], weights[3], weights[5]
    cos_tab, sin_tab = tables
    x, h_one, query_rot, key_rot, values, probs_bf, context, x_mid, h_two, pre_act, act_bf = saved_acts
    num_seq, seq_len, model_dim = x.shape
    num_heads = model_dim // HEAD_DIM
    gb_down = jnp.sum(d_out, axis=(0, 1), dtype=jnp.float32)
    gw_down = jnp.einsum('blf,bld->fd', act_bf, d_out, preferred_element_type=jnp.float32)
    d_act = jnp.einsum('bld,fd->blf', d_out, w_down, preferred_element_type=jnp.float32)
    d_pre = d_act * gelu_slope(pre_act)
    gb_up = jnp.sum(d_pre, axis=(0, 1))
    d_pre_bf = d_pre.astype(jnp.bfloat16)
    gw_up = jnp.einsum('bld,blf->df', h_two, d_pre_bf, preferred_element_type=jnp.float32)
    d_h_two = jnp.einsum('blf,df->bld', d_pre_bf, w_up, preferred_element_type=jnp.float32)
    _, norm_pull_two = jax.vjp(norm_fwd, x_mid.astype(jnp.float32), ln_par[2].astype(jnp.float32), ln_par[3].astype(jnp.float32))
    d_mid_norm, g_gain_two, g_shift_two = norm_pull_two(d_h_two)
    d_mid = (d_out.astype(jnp.float32) + d_mid_norm).astype(jnp.bfloat16)
    gb_out = jnp.sum(d_mid, axis=(0, 1), dtype=jnp.float32)
    gw_out = jnp.einsum('bld,ble->de', context, d_mid, preferred_element_type=jnp.float32)
    d_context = jnp.einsum('ble,de->bld', d_mid, w_attn[3], preferred_element_type=jnp.float32)
    d_context = d_context.astype(jnp.bfloat16).reshape(num_seq, seq_len, num_heads, HEAD_DIM)
    d_probs = jnp.einsum('bqhd,bkhd->bhqk', d_context, values, preferred_element_type=jnp.float32)
    d_values = jnp.einsum('bhqk,bqhd->bkhd', probs_bf, d_context, preferred_element_type=jnp.float32)
    probs_f32 = probs_bf.astype(jnp.float32)
    d_scores = (probs_f32 * (d_probs - jnp.sum(d_probs * probs_f32, axis=-1, keepdims=True))).astype(jnp.bfloat16)
    d_query = jnp.einsum('bhqk,bkhd->bqhd', d_scores, key_rot, preferred_element_type=jnp.float32)
    d_key = jnp.einsum('bhqk,bqhd->bkhd', d_scores, query_rot, preferred_element_type=jnp.float32)
    d_proj = jnp.stack([
        (rotate_back(d_query, cos_tab, sin_tab) * (HEAD_DIM ** -0.5)).astype(jnp.bfloat16),
        rotate_back(d_key, cos_tab, sin_tab).astype(jnp.bfloat16),
        d_values.astype(jnp.bfloat16)]).reshape(3, num_seq, seq_len, model_dim)
    gb_qkv = jnp.sum(d_proj, axis=(1, 2), dtype=jnp.float32)
    gw_qkv = jnp.einsum('bld,kble->kde', h_one, d_proj, preferred_element_type=jnp.float32)
    d_h_one = jnp.einsum('kble,kde->bld', d_proj, w_attn[:3], preferred_element_type=jnp.float32)
    _, norm_pull_one = jax.vjp(norm_fwd, x.astype(jnp.float32), ln_par[0].astype(jnp.float32), ln_par[1].astype(jnp.float32))
    d_x_norm, g_gain_one, g_shift_one = norm_pull_one(d_h_one)
    d_x = (d_mid.astype(jnp.float32) + d_x_norm).astype(jnp.bfloat16)
    gb_attn = jnp.concatenate([gb_qkv, gb_out[None]], axis=0)
    g_ln = jnp.stack([g_gain_one, g_shift_one, g_gain_two, g_shift_two])
    return d_x, (gw_qkv, gw_out, gb_attn, g_ln, gw_up, gb_up, gw_down, gb_down)


BITS = {'c': 1, 'x': 2, 'y': 4, 'z': 8}


def swap(value, axis_name, dim):
    num = 16
    return lax.ppermute(value, axis_name, [(i, i ^ BITS[dim]) for i in range(num)])


def bit_of(axis_name, dim):
    return (lax.axis_index(axis_name) // BITS[dim]) % 2


def gather_rows(shard, axis_name, order):
    me = lax.axis_index(axis_name)
    held = shard[None]
    masks = [0]
    for dim in order:
        got = swap(held, axis_name, dim)
        held = jnp.concatenate([held, got], axis=0)
        masks = masks + [m ^ BITS[dim] for m in masks]
    rows = shard.shape[0]
    out = jnp.zeros((16,) + shard.shape, shard.dtype)
    pos = [masks.index(m) for m in range(16)]
    ordered = jnp.stack([held[p] for p in pos])
    ordered = ordered.reshape((2, 2, 2, 2) + shard.shape)
    for ax, dim in enumerate(('z', 'y', 'x', 'c')):
        flip = bit_of(axis_name, dim)
        ordered = jnp.where(flip == 1, jnp.flip(ordered, ax), ordered)
    return ordered.reshape((16 * rows,) + shard.shape[1:])


def scatter_rows(full, axis_name, order):
    rows = full.shape[0] // 16
    cur = full.reshape((2, 2, 2, 2, rows) + full.shape[1:])
    dims = ['z', 'y', 'x', 'c']
    for dim in order:
        ax = dims.index(dim)
        mine = bit_of(axis_name, dim)
        give = lax.dynamic_index_in_dim(cur, 1 - mine, ax, keepdims=False).astype(jnp.bfloat16)
        keep = lax.dynamic_index_in_dim(cur, mine, ax, keepdims=False)
        cur = keep + swap(give, axis_name, dim).astype(jnp.float32)
        dims.remove(dim)
    return cur


ORDERS = (('x', 'y', 'z', 'c'), ('y', 'z', 'x', 'c'), ('z', 'x', 'y', 'c'))
SORDERS = (('c', 'x', 'y', 'z'), ('c', 'y', 'z', 'x'), ('c', 'z', 'x', 'y'))


def gather_small(layer_shards, axis_name):
    w_attn, b_attn, ln_par, w_up, b_up, w_down, b_down = layer_shards
    packed = jnp.concatenate([b_attn.reshape(-1), ln_par.reshape(-1), b_up, b_down])
    full = lax.all_gather(packed, axis_name)
    n = b_attn.shape[1]
    nu = b_up.shape[0]
    ba = full[:, :4 * n].reshape(16, 4, n).transpose(1, 0, 2).reshape(4, 16 * n)
    lp = full[:, 4 * n:8 * n].reshape(16, 4, n).transpose(1, 0, 2).reshape(4, 16 * n)
    bu = full[:, 8 * n:8 * n + nu].reshape(-1)
    bd = full[:, 8 * n + nu:].reshape(-1)
    return ba, lp, bu, bd


def gather_layer(layer_idx, layer_shards, axis_name):
    w_attn, b_attn, ln_par, w_up, b_up, w_down, b_down = layer_shards
    ba, lp, bu, bd = gather_small(layer_shards, axis_name)
    if layer_idx == 0:
        parts = [gather_rows(w_attn[i], axis_name, ORDERS[i % 3]) for i in range(4)]
        wa = jnp.stack(parts)
        wu = gather_rows(w_up, axis_name, ORDERS[1])
        wd = gather_rows(w_down, axis_name, ORDERS[2])
    else:
        wa = lax.all_gather(w_attn, axis_name, axis=1, tiled=True)
        wu = lax.all_gather(w_up, axis_name, axis=0, tiled=True)
        wd = lax.all_gather(w_down, axis_name, axis=0, tiled=True)
    return (wa, ba, lp, wu, bu, wd, bd)


def scatter_grads(layer_idx, layer_grads, axis_name):
    gw_qkv, gw_out, gb_attn, g_ln, gw_up, gb_up, gw_down, gb_down = layer_grads
    reduce_rows = functools.partial(lax.psum_scatter, axis_name=axis_name, tiled=True)
    if layer_idx == 0:
        attn_part = jnp.stack([scatter_rows(gw_qkv[i], axis_name, SORDERS[i]) for i in range(3)] + [scatter_rows(gw_out, axis_name, SORDERS[0])])
        up_part = scatter_rows(gw_up, axis_name, SORDERS[1])
        down_part = scatter_rows(gw_down, axis_name, SORDERS[2])
    else:
        half = lambda g: g.astype(jnp.bfloat16)
        attn_part = jnp.concatenate([reduce_rows(half(gw_qkv), scatter_dimension=1), reduce_rows(half(gw_out), scatter_dimension=0)[None]], axis=0).astype(jnp.float32)
        up_part = reduce_rows(half(gw_up), scatter_dimension=0).astype(jnp.float32)
        down_part = reduce_rows(half(gw_down), scatter_dimension=0).astype(jnp.float32)
    n = gb_attn.shape[1] // 16
    nu = gb_up.shape[0] // 16
    packed = jnp.concatenate([gb_attn.reshape(4, 16, n).transpose(1, 0, 2).reshape(16, 4 * n),
                              g_ln.reshape(4, 16, n).transpose(1, 0, 2).reshape(16, 4 * n),
                              gb_up.reshape(16, nu), gb_down.reshape(16, n)], axis=1)
    small = lax.psum_scatter(packed, axis_name, scatter_dimension=0, tiled=True)[0]
    return (attn_part, small[:4 * n].reshape(4, n), small[4 * n:8 * n].reshape(4, n), up_part,
            small[8 * n:8 * n + nu], down_part, small[8 * n + nu:])


def solution(mesh):
    axis_name = mesh.axis_names[0]
    batch_spec = P(axis_name)
    weight_specs = (P(None, None, axis_name, None), P(None, None, axis_name), P(None, None, axis_name),
                    P(None, axis_name, None), P(None, axis_name), P(None, axis_name, None), P(None, axis_name))

    def device_step(x, lengths, d_y, w_attn, b_attn, ln_par, w_up, b_up, w_down, b_down):
        shards = (w_attn, b_attn, ln_par, w_up, b_up, w_down, b_down)
        num_layers = w_attn.shape[0]
        tables = rotary_tables(x.shape[1])
        hidden = x
        saved_list = []
        full_list = []
        for layer_idx in range(num_layers):
            full_wts = gather_layer(layer_idx, tuple(shard[layer_idx] for shard in shards), axis_name)
            full_list.append(full_wts)
            hidden, saved_acts = layer_forward(hidden, full_wts, lengths, tables)
            saved_list.append(saved_acts)
        grad_x = d_y
        grads_list = [None] * num_layers
        for layer_idx in reversed(range(num_layers)):
            full_wts = full_list[layer_idx]
            grad_x, layer_grads = layer_backward(grad_x, saved_list[layer_idx], full_wts, tables)
            grads_list[layer_idx] = scatter_grads(layer_idx, layer_grads, axis_name)
        stacked = tuple(jnp.stack([grads_list[layer_pos][field_pos] for layer_pos in range(num_layers)]) for field_pos in range(7))
        return (grad_x,) + stacked

    return jax.shard_map(device_step, mesh=mesh,
                         in_specs=(batch_spec, batch_spec, batch_spec) + weight_specs,
                         out_specs=(batch_spec,) + weight_specs,
                         check_vma=False)
```

```python
import functools, math
import jax
import jax.numpy as jnp
from jax import lax
from jax.experimental import pallas as pl
from jax.experimental.pallas import tpu as pltpu
from jax.sharding import PartitionSpec as P

HEAD_DIM = 64
SEQ = 1024
QT = 256
RB = 64
PAIR = 2 * HEAD_DIM
NEG_BIG = -1e30
NN = (((1,), (0,)), ((), ()))
NT = (((1,), (1,)), ((), ()))
TN = (((0,), (0,)), ((), ()))


def dot(a, b, dims):
    return lax.dot_general(a, b, dims, preferred_element_type=jnp.float32)


def lane_iota(rows):
    return lax.broadcasted_iota(jnp.int32, (rows, PAIR), 1)


def attn_fwd_kernel(len_ref, q_ref, k_ref, v_ref, ctx_ref, p_ref, ka_ref, qa_ref, vt_ref, e_ref, top_ref, sum_ref, ctxt_ref):
    seq_len = len_ref[pl.program_id(0)]
    lane = lane_iota(1)
    hidden_key = lax.broadcasted_iota(jnp.int32, (SEQ, PAIR), 0) >= seq_len
    for h in range(2):
        mine = (lane // HEAD_DIM) == h
        aux = lane == (1 - h) * HEAD_DIM
        own = mine.astype(jnp.float32).astype(jnp.bfloat16)
        one = aux.astype(jnp.float32).astype(jnp.bfloat16)
        bar = jnp.where(aux, NEG_BIG, 0.0).astype(jnp.bfloat16)
        ka_ref[h] = jnp.where(hidden_key, jnp.broadcast_to(bar, (SEQ, PAIR)), k_ref[...] * own)
        qa_ref[h] = q_ref[...] * own + one
    vt_ref[...] = v_ref[...].T
    def at(t):
        return pl.ds(pl.multiple_of(t * QT, QT), QT)

    def fold(x, op):
        while x.shape[0] > 8:
            half = x.shape[0] // 2
            x = op(x[:half], x[half:])
        return x

    def spread(x):
        return jnp.concatenate([x] * (RB // 8), axis=0)

    def rise(t, h):
        s = dot(ka_ref[h], qa_ref[h, at(t)], NT)
        for c in range(SEQ // RB):
            part = s[c * RB:(c + 1) * RB]
            top = fold(part, jnp.maximum)
            e = jnp.exp(part - spread(top))
            e_ref[h, c * RB:(c + 1) * RB] = e
            top_ref[h, c * 8:(c + 1) * 8] = top
            sum_ref[h, c * 8:(c + 1) * 8] = fold(e, jnp.add)

    def settle(t, h):
        tops = top_ref[h]
        weight = jnp.exp(tops - jnp.max(tops, axis=0, keepdims=True))
        scale = weight * (1.0 / jnp.sum(weight * sum_ref[h], axis=0, keepdims=True))
        for c in range(SEQ // RB):
            p_ref[h, c * RB:(c + 1) * RB, at(t)] = (e_ref[h, c * RB:(c + 1) * RB] * spread(scale[c * 8:(c + 1) * 8])).astype(jnp.bfloat16)
        rows = slice(h * HEAD_DIM, (h + 1) * HEAD_DIM)
        ctxt_ref[rows, at(t)] = dot(vt_ref[rows], p_ref[h, :, at(t)], NN)

    last = SEQ // QT - 1
    rise(0, 0)

    def turn(t, _):
        settle(t, 0)
        rise(t, 1)
        rise(jnp.minimum(t + 1, last), 0)
        settle(t, 1)
        return 0

    lax.fori_loop(0, SEQ // QT, turn, 0)
    ctx_ref[...] = ctxt_ref[...].T.astype(jnp.bfloat16)


def attn_fwd(lengths, q, k, v):
    tokens, width = q.shape
    seqs, pairs = tokens // SEQ, width // PAIR
    spec = pl.BlockSpec((SEQ, PAIR), lambda b, h, n: (b, h))
    return pl.pallas_call(
        attn_fwd_kernel,
        grid_spec=pltpu.PrefetchScalarGridSpec(
            num_scalar_prefetch=1, grid=(seqs, pairs),
            in_specs=[spec, spec, spec],
            out_specs=[spec, pl.BlockSpec((None, 2, SEQ, SEQ), lambda b, h, n: (b, h, 0, 0))],
            scratch_shapes=[pltpu.VMEM((2, SEQ, PAIR), jnp.bfloat16), pltpu.VMEM((2, SEQ, PAIR), jnp.bfloat16),
                            pltpu.VMEM((PAIR, SEQ), jnp.bfloat16), pltpu.VMEM((2, SEQ, QT), jnp.float32), pltpu.VMEM((2, SEQ // RB * 8, QT), jnp.float32), pltpu.VMEM((2, SEQ // RB * 8, QT), jnp.float32),
                            pltpu.VMEM((PAIR, SEQ), jnp.float32)]),
        out_shape=[jax.ShapeDtypeStruct((tokens, width), jnp.bfloat16),
                   jax.ShapeDtypeStruct((seqs, 2 * pairs, SEQ, SEQ), jnp.bfloat16)],
        compiler_params=pltpu.CompilerParams(dimension_semantics=("arbitrary", "arbitrary"), vmem_limit_bytes=56 << 20),
        cost_estimate=pl.CostEstimate(flops=4 * tokens * SEQ * width * 4, bytes_accessed=90 << 20, transcendentals=tokens * SEQ * 16),
        name='attn_fwd',
    )(lengths, q, k, v)


def spin(x, cos, sin, sign):
    half = HEAD_DIM // 2
    low = (lax.broadcasted_iota(jnp.int32, x.shape, 1) % HEAD_DIM) < half
    other = jnp.where(low, pltpu.roll(x, PAIR - half, 1), pltpu.roll(x, half, 1))
    return x * cos + other * (sin * sign)


def attn_bwd_kernel(len_ref, q_ref, k_ref, v_ref, o_ref, do_ref, p_ref, cos_ref, sin_ref, dq_ref, dk_ref, dv_ref,
                    doh_ref, qh_ref, kt_ref, d_ref, ds_ref, dqt_ref):
    lane = lane_iota(1)
    for h in range(2):
        own = ((lane // HEAD_DIM) == h).astype(jnp.float32).astype(jnp.bfloat16)
        doh_ref[h] = do_ref[...] * own
        qh_ref[h] = q_ref[...] * own
    kt_ref[...] = k_ref[...].T
    prod = (do_ref[...].astype(jnp.float32) * o_ref[...].astype(jnp.float32)).T
    for h in range(2):
        d_ref[h:h + 1] = jnp.sum(prod[h * HEAD_DIM:(h + 1) * HEAD_DIM], axis=0, keepdims=True)
    for h in range(2):
        for t in range(SEQ // QT):
            cols = slice(t * QT, (t + 1) * QT)
            dp = dot(v_ref[...], doh_ref[h, cols], NT)
            ds_ref[h, :, cols] = (p_ref[h, :, cols].astype(jnp.float32) * (dp - d_ref[h:h + 1, cols])).astype(jnp.bfloat16)
    dv_ref[...] = (dot(p_ref[0], doh_ref[0], NN) + dot(p_ref[1], doh_ref[1], NN)).astype(jnp.bfloat16)
    for h in range(2):
        dqt_ref[h * HEAD_DIM:(h + 1) * HEAD_DIM] = dot(kt_ref[h * HEAD_DIM:(h + 1) * HEAD_DIM], ds_ref[h], NN)
    dk = dot(ds_ref[0], qh_ref[0], NN) + dot(ds_ref[1], qh_ref[1], NN)
    dk_ref[...] = spin(dk, cos_ref[...], sin_ref[...], -1.0).astype(jnp.bfloat16)
    dq_ref[...] = (spin(dqt_ref[...].T, cos_ref[...], sin_ref[...], -1.0) * (HEAD_DIM ** -0.5)).astype(jnp.bfloat16)


def attn_bwd(lengths, q, k, v, ctx, d_ctx, probs, cos_tab, sin_tab):
    tokens, width = q.shape
    seqs, pairs = tokens // SEQ, width // PAIR
    spec = pl.BlockSpec((SEQ, PAIR), lambda b, h, n: (b, h))
    table = pl.BlockSpec((SEQ, PAIR), lambda b, h, n: (0, 0))
    return pl.pallas_call(
        attn_bwd_kernel,
        grid_spec=pltpu.PrefetchScalarGridSpec(
            num_scalar_prefetch=1, grid=(seqs, pairs),
            in_specs=[spec] * 5 + [pl.BlockSpec((None, 2, SEQ, SEQ), lambda b, h, n: (b, h, 0, 0)), table, table],
            out_specs=[spec] * 3,
            scratch_shapes=[pltpu.VMEM((2, SEQ, PAIR), jnp.bfloat16), pltpu.VMEM((2, SEQ, PAIR), jnp.bfloat16),
                            pltpu.VMEM((PAIR, SEQ), jnp.bfloat16), pltpu.VMEM((8, SEQ), jnp.float32),
                            pltpu.VMEM((2, SEQ, SEQ), jnp.bfloat16), pltpu.VMEM((PAIR, SEQ), jnp.float32)]),
        out_shape=[jax.ShapeDtypeStruct((tokens, width), jnp.bfloat16)] * 3,
        compiler_params=pltpu.CompilerParams(dimension_semantics=("arbitrary", "arbitrary"), vmem_limit_bytes=56 << 20),
        cost_estimate=pl.CostEstimate(flops=8 * tokens * SEQ * width * 4, bytes_accessed=100 << 20, transcendentals=0),
        name='attn_bwd',
    )(lengths, q, k, v, ctx, d_ctx, probs, cos_tab, sin_tab)


EPS = 1e-5
THETA = 10000.0
HIGH = 60 << 20


def whole(shape):
    return pl.BlockSpec(shape, lambda *i: (0,) * len(shape), pipeline_mode=pl.Buffered(1))


def partial(shape):
    return pl.BlockSpec(shape, lambda *i: (0,) * len(shape))


def rows_of(block, width):
    return pl.BlockSpec((block, width), lambda i: (i, 0))


def params(*semantics):
    return pltpu.CompilerParams(dimension_semantics=semantics or ('arbitrary',), vmem_limit_bytes=HIGH)


def cost(flops, moved):
    return pl.CostEstimate(flops=flops, bytes_accessed=moved, transcendentals=0)


def normal(x):
    mean = jnp.mean(x, axis=-1, keepdims=True)
    centered = x - mean
    inv = lax.rsqrt(jnp.mean(centered * centered, axis=-1, keepdims=True) + EPS)
    return centered * inv, inv


def norm_back(x, gain, grad):
    unit, inv = normal(x)
    scaled = grad * gain
    inner = scaled - jnp.mean(scaled, axis=-1, keepdims=True) - unit * jnp.mean(scaled * unit, axis=-1, keepdims=True)
    return inv * inner, unit


def eights(x):
    return jnp.sum(x.reshape(x.shape[0] // 8, 8, x.shape[1]), axis=0)


def add_up(ref, value):
    first = pl.program_id(0) == 0

    @pl.when(first)
    def _():
        ref[...] = value

    @pl.when(jnp.logical_not(first))
    def _():
        ref[...] += value


def qkv_kernel(x_ref, w_ref, b_ref, ln_ref, cos_ref, sin_ref, h_ref, q_ref, k_ref, v_ref):
    unit, _ = normal(x_ref[...].astype(jnp.float32))
    h_ref[...] = (unit * ln_ref[0:1] + ln_ref[1:2]).astype(jnp.bfloat16)
    for j, out_ref in enumerate((q_ref, k_ref, v_ref)):
        full = dot(h_ref[...], w_ref[j], NN) + b_ref[j:j + 1]
        if j == 2:
            out_ref[...] = full.astype(jnp.bfloat16)
            continue
        if j == 0:
            full = full * (HEAD_DIM ** -0.5)
        for c in range(0, full.shape[1], PAIR):
            out_ref[:, c:c + PAIR] = spin(full[:, c:c + PAIR], cos_ref[...], sin_ref[...], 1.0).astype(jnp.bfloat16)


def qkv(x, w, b, ln, cos, sin):
    tokens, width = x.shape
    block = 512
    row = rows_of(block, width)
    table = pl.BlockSpec((block, PAIR), lambda i: (i % (SEQ // block), 0))
    return pl.pallas_call(
        qkv_kernel, grid=(tokens // block,),
        in_specs=[row, whole(w.shape), whole(b.shape), whole(ln.shape), table, table],
        out_specs=[row] * 4,
        out_shape=[jax.ShapeDtypeStruct(x.shape, jnp.bfloat16)] * 4,
        compiler_params=params(), cost_estimate=cost(6 * tokens * width * width, 26 << 20), name='qkv',
    )(x, w, b, ln, cos, sin)


def out_kernel(ctx_ref, x_ref, w_ref, b_ref, ln_ref, mid_ref, h_ref):
    mid = (x_ref[...].astype(jnp.float32) + dot(ctx_ref[...], w_ref[...], NN) + b_ref[...]).astype(jnp.bfloat16)
    mid_ref[...] = mid
    unit, _ = normal(mid.astype(jnp.float32))
    h_ref[...] = (unit * ln_ref[2:3] + ln_ref[3:4]).astype(jnp.bfloat16)


def out_proj(ctx, x, w, b, ln):
    tokens, width = x.shape
    block = 512
    row = rows_of(block, width)
    return pl.pallas_call(
        out_kernel, grid=(tokens // block,),
        in_specs=[row, row, whole(w.shape), whole(b.shape), whole(ln.shape)], out_specs=[row] * 2,
        out_shape=[jax.ShapeDtypeStruct(x.shape, jnp.bfloat16)] * 2,
        compiler_params=params(), cost_estimate=cost(2 * tokens * width * width, 18 << 20), name='out_proj',
    )(ctx, x, w, b, ln)


def mlp_kernel(h_ref, mid_ref, wu_ref, bu_ref, wd_ref, bd_ref, act_ref, slope_ref, y_ref):
    total = mid_ref[...].astype(jnp.float32) + bd_ref[...]
    wide = wu_ref.shape[1]
    for c in range(0, wide, 1024):
        cols = slice(c, c + 1024)
        pre = dot(h_ref[...], wu_ref[:, cols], NN) + bu_ref[:, cols]
        cdf = 0.5 + 0.5 * lax.erf(pre * (1.0 / math.sqrt(2.0)))
        act_ref[:, cols] = (pre * cdf).astype(jnp.bfloat16)
        slope_ref[:, cols] = cdf + pre * (jnp.exp(-0.5 * pre * pre) * (1.0 / math.sqrt(2.0 * math.pi)))
        total = total + dot(act_ref[:, cols], wd_ref[cols], NN)
    y_ref[...] = total.astype(jnp.bfloat16)


def mlp(h, mid, wu, bu, wd, bd):
    tokens, width = h.shape
    wide = wu.shape[1]
    block = 256
    row, long = rows_of(block, width), rows_of(block, wide)
    return pl.pallas_call(
        mlp_kernel, grid=(tokens // block,),
        in_specs=[row, row, whole(wu.shape), whole(bu.shape), whole(wd.shape), whole(bd.shape)],
        out_specs=[long, long, row],
        out_shape=[jax.ShapeDtypeStruct((tokens, wide), jnp.bfloat16), jax.ShapeDtypeStruct((tokens, wide), jnp.float32),
                   jax.ShapeDtypeStruct(h.shape, jnp.bfloat16)],
        compiler_params=params(), cost_estimate=cost(4 * tokens * width * wide, 80 << 20), name='mlp',
    )(h, mid, wu, bu, wd, bd)


def mlp_back_kernel(dy_ref, slope_ref, wd_ref, wu_ref, mid_ref, ln_ref, wo_ref,
                    dpre_ref, dmid_ref, dctx_ref, gbu_ref, gln_ref):
    dy = dy_ref[...]
    grad = None
    wide = wu_ref.shape[1]
    first = pl.program_id(0) == 0

    @pl.when(first)
    def _():
        gbu_ref[...] = jnp.zeros_like(gbu_ref)
        gln_ref[...] = jnp.zeros_like(gln_ref)

    for c in range(0, wide, 1024):
        cols = slice(c, c + 1024)
        dpre = dot(dy, wd_ref[cols], NT) * slope_ref[:, cols]
        gbu_ref[:, cols] += eights(dpre)
        dpre_ref[:, cols] = dpre.astype(jnp.bfloat16)
        part = dot(dpre_ref[:, cols], wu_ref[:, cols], NT)
        grad = part if grad is None else grad + part
    dy = dy.astype(jnp.float32)
    back, unit = norm_back(mid_ref[...].astype(jnp.float32), ln_ref[2:3], grad)
    dmid = (dy + back).astype(jnp.bfloat16)
    dmid_ref[...] = dmid
    gln_ref[0:8] += eights(grad * unit)
    gln_ref[8:16] += eights(grad)
    gln_ref[16:24] += eights(dmid.astype(jnp.float32))
    gln_ref[24:32] += eights(dy)
    dctx_ref[...] = dot(dmid, wo_ref[...], NT).astype(jnp.bfloat16)


def mlp_back(dy, slope, wd, wu, mid, ln, wo):
    tokens, width = dy.shape
    wide = wu.shape[1]
    block = 256
    row, long = rows_of(block, width), rows_of(block, wide)
    half = jax.ShapeDtypeStruct(dy.shape, jnp.bfloat16)
    return pl.pallas_call(
        mlp_back_kernel, grid=(tokens // block,),
        in_specs=[row, long, whole(wd.shape), whole(wu.shape), row, whole(ln.shape), whole(wo.shape)],
        out_specs=[long, row, row, partial((8, wide)), partial((32, width))],
        out_shape=[jax.ShapeDtypeStruct((tokens, wide), jnp.bfloat16), half, half,
                   jax.ShapeDtypeStruct((8, wide), jnp.float32), jax.ShapeDtypeStruct((32, width), jnp.float32)],
        compiler_params=params(), cost_estimate=cost(2 * tokens * width * (2 * wide + width), 90 << 20), name='mlp_back',
    )(dy, slope, wd, wu, mid, ln, wo)


def in_back_kernel(dq_ref, dk_ref, dv_ref, w_ref, x_ref, ln_ref, dmid_ref, dx_ref, gln_ref):
    @pl.when(pl.program_id(0) == 0)
    def _():
        gln_ref[...] = jnp.zeros_like(gln_ref)

    grad = dot(dq_ref[...], w_ref[0], NT) + dot(dk_ref[...], w_ref[1], NT) + dot(dv_ref[...], w_ref[2], NT)
    back, unit = norm_back(x_ref[...].astype(jnp.float32), ln_ref[0:1], grad)
    dx_ref[...] = (dmid_ref[...].astype(jnp.float32) + back).astype(jnp.bfloat16)
    gln_ref[0:8] += eights(grad * unit)
    gln_ref[8:16] += eights(grad)


def in_back(dq, dk, dv, w, x, ln, dmid):
    tokens, width = x.shape
    block = 512
    row = rows_of(block, width)
    return pl.pallas_call(
        in_back_kernel, grid=(tokens // block,),
        in_specs=[row, row, row, whole(w.shape), row, whole(ln.shape), row],
        out_specs=[row, partial((16, width))],
        out_shape=[jax.ShapeDtypeStruct(x.shape, jnp.bfloat16), jax.ShapeDtypeStruct((16, width), jnp.float32)],
        compiler_params=params(), cost_estimate=cost(6 * tokens * width * width, 34 << 20), name='in_back',
    )(dq, dk, dv, w, x, ln, dmid)


def grad_kernel(a_ref, b_ref, g_ref):
    g_ref[...] = dot(a_ref[...], b_ref[...], TN).astype(jnp.bfloat16)


def weight_grad(a, b, name, tall):
    tokens, m = a.shape
    n = b.shape[1]
    block = 512
    if tall:
        grid, a_spec, b_spec = (m // block,), pl.BlockSpec((tokens, block), lambda i: (0, i)), whole(b.shape)
        out = pl.BlockSpec((block, n), lambda i: (i, 0))
    else:
        grid, a_spec, b_spec = (n // block,), whole(a.shape), pl.BlockSpec((tokens, block), lambda i: (0, i))
        out = pl.BlockSpec((m, block), lambda i: (0, i))
    return pl.pallas_call(
        grad_kernel, grid=grid, in_specs=[a_spec, b_spec], out_specs=out,
        out_shape=jax.ShapeDtypeStruct((m, n), jnp.bfloat16),
        compiler_params=params(), cost_estimate=cost(2 * tokens * m * n, 2 * (tokens * (m + n) + m * n)), name=name,
    )(a, b)


def qkv_grad_kernel(h_ref, dq_ref, dk_ref, dv_ref, g_ref, gb_ref):
    for j, d_ref in enumerate((dq_ref, dk_ref, dv_ref)):
        g_ref[j] = dot(h_ref[...], d_ref[...], TN).astype(jnp.bfloat16)
        gb_ref[8 * j:8 * j + 8] = eights(d_ref[...].astype(jnp.float32))


def qkv_grad(h, dq, dk, dv):
    tokens, width = h.shape
    block = 256
    cols = pl.BlockSpec((tokens, block), lambda i: (0, i))
    return pl.pallas_call(
        qkv_grad_kernel, grid=(width // block,),
        in_specs=[whole(h.shape), cols, cols, cols],
        out_specs=[pl.BlockSpec((3, width, block), lambda i: (0, 0, i)), pl.BlockSpec((24, block), lambda i: (0, i))],
        out_shape=[jax.ShapeDtypeStruct((3, width, width), jnp.bfloat16), jax.ShapeDtypeStruct((24, width), jnp.float32)],
        compiler_params=params(), cost_estimate=cost(6 * tokens * width * width, 24 << 20), name='qkv_grad',
    )(h, dq, dk, dv)


def rotary_tables():
    half = HEAD_DIM // 2
    inv_freq = 1.0 / (THETA ** (jnp.arange(half, dtype=jnp.float32) * (2.0 / HEAD_DIM)))
    angles = jnp.arange(SEQ, dtype=jnp.float32)[:, None] * inv_freq[None, :]
    cos, sin = jnp.cos(angles), jnp.sin(angles)
    return jnp.concatenate([cos] * 4, axis=1), jnp.concatenate([-sin, sin, -sin, sin], axis=1)


BITS = {'c': 1, 'x': 2, 'y': 4, 'z': 8}


def swap(value, axis_name, dim):
    return lax.ppermute(value, axis_name, [(i, i ^ BITS[dim]) for i in range(16)])


def bit_of(axis_name, dim):
    return (lax.axis_index(axis_name) // BITS[dim]) % 2


def gather_packed(packed, axis_name):
    held = packed[None]
    for dim in ('c', 'x', 'y', 'z'):
        got = swap(held, axis_name, dim)
        mine = bit_of(axis_name, dim)
        held = jnp.where(mine == 0, jnp.concatenate([held, got]), jnp.concatenate([got, held]))
    return held


def scatter_packed(full, axis_name):
    cur = full
    for dim in ('z', 'y', 'x', 'c'):
        mine = bit_of(axis_name, dim)
        half = cur.shape[0] // 2
        low, high = cur[:half], cur[half:]
        give = jnp.where(mine == 0, high, low)
        keep = jnp.where(mine == 0, low, high)
        cur = keep + swap(give, axis_name, dim)
    return cur[0]


def pack_params(b_attn, ln_par, b_up, b_down):
    layers = b_attn.shape[0]
    flat = jnp.concatenate([b_attn.reshape(layers, -1), ln_par.reshape(layers, -1), b_up, b_down], axis=1)
    return flat


def unpack_params(full, layer, n, nu):
    part = full[:, layer].astype(jnp.float32)
    b_attn = part[:, :4 * n].reshape(16, 4, n).transpose(1, 0, 2).reshape(4, 16 * n)
    ln = part[:, 4 * n:8 * n].reshape(16, 4, n).transpose(1, 0, 2).reshape(4, 16 * n)
    b_up = part[:, 8 * n:8 * n + nu].reshape(1, 16 * nu)
    b_down = part[:, 8 * n + nu:].reshape(1, 16 * n)
    return b_attn, ln, b_up, b_down


def solution(mesh):
    axis_name = mesh.axis_names[0]
    batch_spec = P(axis_name)
    weight_specs = (P(None, None, axis_name, None), P(None, None, axis_name), P(None, None, axis_name),
                    P(None, axis_name, None), P(None, axis_name), P(None, axis_name, None), P(None, axis_name))

    def device_step(x, lengths, d_y, w_attn, b_attn, ln_par, w_up, b_up, w_down, b_down):
        layers = w_attn.shape[0]
        seqs, seq_len, width = x.shape
        tokens = seqs * seq_len
        n, nu = b_attn.shape[2], b_up.shape[1]
        cos, sin = rotary_tables()
        gather = functools.partial(lax.all_gather, axis_name=axis_name, tiled=True)
        scatter = functools.partial(lax.psum_scatter, axis_name=axis_name, tiled=True)
        small = gather_packed(pack_params(b_attn, ln_par, b_up, b_down), axis_name)
        hidden = x.reshape(tokens, width)
        saved = []
        for l in range(layers):
            ba, ln, bu, bd = unpack_params(small, l, n, nu)
            wqkv = gather(w_attn[l, :3], axis=1)
            wo = gather(w_attn[l, 3], axis=0)
            wu = gather(w_up[l], axis=0)
            wd = gather(w_down[l], axis=0)
            h_one, q, k, v = qkv(hidden, wqkv, ba[:3], ln, cos, sin)
            ctx, probs = attn_fwd(lengths, q, k, v)
            mid, h_two = out_proj(ctx, hidden, wo, ba[3:4], ln)
            act, slope, out = mlp(h_two, mid, wu, bu, wd, bd)
            saved.append((hidden, h_one, q, k, v, ctx, probs, mid, h_two, act, slope, wqkv, wo, wu, wd, ln))
            hidden = out
        grad = d_y.reshape(tokens, width)
        grads = [None] * layers
        for l in reversed(range(layers)):
            x_in, h_one, q, k, v, ctx, probs, mid, h_two, act, slope, wqkv, wo, wu, wd, ln = saved[l]
            after = lax.optimization_barrier
            gw_down, grad = after((weight_grad(act, grad, 'down_grad', True), grad))
            g_down = scatter(gw_down, scatter_dimension=0)
            d_pre, d_mid, d_ctx, gb_up, gln_two = mlp_back(grad, slope, wd, wu, mid, ln, wo)
            if l + 1 < layers:
                above, h_two = after((grads[l + 1][0], h_two))
                grads[l + 1] = (above,) + grads[l + 1][1:]
            gw_up, gw_out, d_ctx = after((weight_grad(h_two, d_pre, 'up_grad', False), weight_grad(ctx, d_mid, 'out_grad', False), d_ctx))
            g_up = scatter(gw_up, scatter_dimension=0)
            g_out = scatter(gw_out, scatter_dimension=0)
            dq, dk, dv = attn_bwd(lengths, q, k, v, ctx, d_ctx, probs, cos, sin)
            g_down, dq = after((g_down, dq))
            gw, gb_qkv = qkv_grad(h_one, dq, dk, dv)
            gw, dq, g_up = after((gw, dq, g_up))
            g_qkv = scatter(gw, scatter_dimension=1)
            grad, gln_one = in_back(dq, dk, dv, wqkv, x_in, ln, d_mid)
            g_out, grad = after((g_out, grad))
            sums_two = jnp.sum(gln_two.reshape(4, 8, width), axis=1)
            sums_one = jnp.sum(gln_one.reshape(2, 8, width), axis=1)
            gb_three = jnp.sum(gb_qkv.reshape(3, 8, width), axis=1)
            gb_wide = jnp.sum(gb_up, axis=0)
            by_dev = lambda s: s.reshape(-1, 16, n).transpose(1, 0, 2).reshape(16, -1)
            packed = jnp.concatenate([by_dev(gb_three), by_dev(sums_two[2:3]), by_dev(sums_one), by_dev(sums_two[:2]),
                                      gb_wide.reshape(16, nu), by_dev(sums_two[3:4])], axis=1)
            grads[l] = ((g_qkv, g_out), g_up, g_down, packed)
        got = scatter_packed(jnp.stack([g[3] for g in grads], axis=1), axis_name)
        f32 = lambda g: g.astype(jnp.float32)
        g_attn = jnp.stack([jnp.concatenate([f32(g[0][0]), f32(g[0][1])[None]]) for g in grads])
        g_up = jnp.stack([f32(g[1]) for g in grads])
        g_down = jnp.stack([f32(g[2]) for g in grads])
        return (grad.reshape(x.shape), g_attn, got[:, :4 * n].reshape(layers, 4, n), got[:, 4 * n:8 * n].reshape(layers, 4, n),
                g_up, got[:, 8 * n:8 * n + nu], g_down, got[:, 8 * n + nu:])

    return jax.shard_map(device_step, mesh=mesh,
                         in_specs=(batch_spec, batch_spec, batch_spec) + weight_specs,
                         out_specs=(batch_spec,) + weight_specs,
                         check_vma=False)
```

```python
import functools, math
import jax
import jax.numpy as jnp
from jax import lax
from jax.experimental import pallas as pl
from jax.experimental.pallas import tpu as pltpu
from jax.sharding import PartitionSpec as P

HEAD_DIM = 64
SEQ = 1024
QT = 256
RB = 64
PAIR = 2 * HEAD_DIM
NEG_BIG = -1e30
NN = (((1,), (0,)), ((), ()))
NT = (((1,), (1,)), ((), ()))
TN = (((0,), (0,)), ((), ()))


def dot(a, b, dims):
    return lax.dot_general(a, b, dims, preferred_element_type=jnp.float32)


def lane_iota(rows):
    return lax.broadcasted_iota(jnp.int32, (rows, PAIR), 1)


def attn_fwd_kernel(len_ref, q_ref, k_ref, v_ref, ctx_ref, p_ref, ka_ref, qa_ref, vt_ref, e_ref, top_ref, sum_ref, ctxt_ref):
    seq_len = len_ref[pl.program_id(0)]
    lane = lane_iota(1)
    hidden_key = lax.broadcasted_iota(jnp.int32, (SEQ, PAIR), 0) >= seq_len
    for h in range(2):
        mine = (lane // HEAD_DIM) == h
        aux = lane == (1 - h) * HEAD_DIM
        own = mine.astype(jnp.float32).astype(jnp.bfloat16)
        one = aux.astype(jnp.float32).astype(jnp.bfloat16)
        bar = jnp.where(aux, NEG_BIG, 0.0).astype(jnp.bfloat16)
        ka_ref[h] = jnp.where(hidden_key, jnp.broadcast_to(bar, (SEQ, PAIR)), k_ref[...] * own)
        qa_ref[h] = q_ref[...] * own + one
    vt_ref[...] = v_ref[...].T

    def at(t):
        return pl.ds(pl.multiple_of(t * QT, QT), QT)

    def fold(x, op):
        while x.shape[0] > 8:
            half = x.shape[0] // 2
            x = op(x[:half], x[half:])
        return x

    def spread(x):
        return jnp.concatenate([x] * (RB // 8), axis=0)

    def rise(t, h):
        s = dot(ka_ref[h], qa_ref[h, at(t)], NT)
        for c in range(SEQ // RB):
            part = s[c * RB:(c + 1) * RB]
            top = fold(part, jnp.maximum)
            e = jnp.exp(part - spread(top))
            e_ref[h, c * RB:(c + 1) * RB] = e
            top_ref[h, c * 8:(c + 1) * 8] = top
            sum_ref[h, c * 8:(c + 1) * 8] = fold(e, jnp.add)

    def settle(t, h):
        tops = top_ref[h]
        weight = jnp.exp(tops - jnp.max(tops, axis=0, keepdims=True))
        scale = weight * (1.0 / jnp.sum(weight * sum_ref[h], axis=0, keepdims=True))
        for c in range(SEQ // RB):
            p_ref[h, c * RB:(c + 1) * RB, at(t)] = (e_ref[h, c * RB:(c + 1) * RB] * spread(scale[c * 8:(c + 1) * 8])).astype(jnp.bfloat16)
        rows = slice(h * HEAD_DIM, (h + 1) * HEAD_DIM)
        ctxt_ref[rows, at(t)] = dot(vt_ref[rows], p_ref[h, :, at(t)], NN)

    last = SEQ // QT - 1
    rise(0, 0)

    def turn(t, _):
        settle(t, 0)
        rise(t, 1)
        rise(jnp.minimum(t + 1, last), 0)
        settle(t, 1)
        return 0

    lax.fori_loop(0, SEQ // QT, turn, 0)
    ctx_ref[...] = ctxt_ref[...].T.astype(jnp.bfloat16)


def attn_fwd(lengths, q, k, v):
    tokens, width = q.shape
    seqs, pairs = tokens // SEQ, width // PAIR
    spec = pl.BlockSpec((SEQ, PAIR), lambda b, h, n: (b, h))
    return pl.pallas_call(
        attn_fwd_kernel,
        grid_spec=pltpu.PrefetchScalarGridSpec(
            num_scalar_prefetch=1, grid=(seqs, pairs),
            in_specs=[spec, spec, spec],
            out_specs=[spec, pl.BlockSpec((None, 2, SEQ, SEQ), lambda b, h, n: (b, h, 0, 0))],
            scratch_shapes=[pltpu.VMEM((2, SEQ, PAIR), jnp.bfloat16), pltpu.VMEM((2, SEQ, PAIR), jnp.bfloat16),
                            pltpu.VMEM((PAIR, SEQ), jnp.bfloat16), pltpu.VMEM((2, SEQ, QT), jnp.float32), pltpu.VMEM((2, SEQ // RB * 8, QT), jnp.float32), pltpu.VMEM((2, SEQ // RB * 8, QT), jnp.float32),
                            pltpu.VMEM((PAIR, SEQ), jnp.float32)]),
        out_shape=[jax.ShapeDtypeStruct((tokens, width), jnp.bfloat16),
                   jax.ShapeDtypeStruct((seqs, 2 * pairs, SEQ, SEQ), jnp.bfloat16)],
        compiler_params=pltpu.CompilerParams(dimension_semantics=("arbitrary", "arbitrary"), vmem_limit_bytes=56 << 20),
        cost_estimate=pl.CostEstimate(flops=4 * tokens * SEQ * width * 4, bytes_accessed=90 << 20, transcendentals=tokens * SEQ * 16),
        name='attn_fwd',
    )(lengths, q, k, v)


def spin(x, cos, sin, sign):
    half = HEAD_DIM // 2
    low = (lax.broadcasted_iota(jnp.int32, x.shape, 1) % HEAD_DIM) < half
    other = jnp.where(low, pltpu.roll(x, PAIR - half, 1), pltpu.roll(x, half, 1))
    return x * cos + other * (sin * sign)


def attn_bwd_kernel(len_ref, q_ref, k_ref, v_ref, o_ref, do_ref, p_ref, cos_ref, sin_ref, dq_ref, dk_ref, dv_ref,
                    doh_ref, qh_ref, kt_ref, d_ref, ds_ref, dqt_ref):
    lane = lane_iota(1)
    for h in range(2):
        own = ((lane // HEAD_DIM) == h).astype(jnp.float32).astype(jnp.bfloat16)
        doh_ref[h] = do_ref[...] * own
        qh_ref[h] = q_ref[...] * own
    kt_ref[...] = k_ref[...].T
    prod = (do_ref[...].astype(jnp.float32) * o_ref[...].astype(jnp.float32)).T
    for h in range(2):
        d_ref[h:h + 1] = jnp.sum(prod[h * HEAD_DIM:(h + 1) * HEAD_DIM], axis=0, keepdims=True)
    for h in range(2):
        for t in range(SEQ // QT):
            cols = slice(t * QT, (t + 1) * QT)
            dp = dot(v_ref[...], doh_ref[h, cols], NT)
            ds_ref[h, :, cols] = (p_ref[h, :, cols].astype(jnp.float32) * (dp - d_ref[h:h + 1, cols])).astype(jnp.bfloat16)
    dv_ref[...] = (dot(p_ref[0], doh_ref[0], NN) + dot(p_ref[1], doh_ref[1], NN)).astype(jnp.bfloat16)
    for h in range(2):
        dqt_ref[h * HEAD_DIM:(h + 1) * HEAD_DIM] = dot(kt_ref[h * HEAD_DIM:(h + 1) * HEAD_DIM], ds_ref[h], NN)
    dk = dot(ds_ref[0], qh_ref[0], NN) + dot(ds_ref[1], qh_ref[1], NN)
    dk_ref[...] = spin(dk, cos_ref[...], sin_ref[...], -1.0).astype(jnp.bfloat16)
    dq_ref[...] = (spin(dqt_ref[...].T, cos_ref[...], sin_ref[...], -1.0) * (HEAD_DIM ** -0.5)).astype(jnp.bfloat16)


def attn_bwd(lengths, q, k, v, ctx, d_ctx, probs, cos_tab, sin_tab):
    tokens, width = q.shape
    seqs, pairs = tokens // SEQ, width // PAIR
    spec = pl.BlockSpec((SEQ, PAIR), lambda b, h, n: (b, h))
    table = pl.BlockSpec((SEQ, PAIR), lambda b, h, n: (0, 0))
    return pl.pallas_call(
        attn_bwd_kernel,
        grid_spec=pltpu.PrefetchScalarGridSpec(
            num_scalar_prefetch=1, grid=(seqs, pairs),
            in_specs=[spec] * 5 + [pl.BlockSpec((None, 2, SEQ, SEQ), lambda b, h, n: (b, h, 0, 0)), table, table],
            out_specs=[spec] * 3,
            scratch_shapes=[pltpu.VMEM((2, SEQ, PAIR), jnp.bfloat16), pltpu.VMEM((2, SEQ, PAIR), jnp.bfloat16),
                            pltpu.VMEM((PAIR, SEQ), jnp.bfloat16), pltpu.VMEM((8, SEQ), jnp.float32),
                            pltpu.VMEM((2, SEQ, SEQ), jnp.bfloat16), pltpu.VMEM((PAIR, SEQ), jnp.float32)]),
        out_shape=[jax.ShapeDtypeStruct((tokens, width), jnp.bfloat16)] * 3,
        compiler_params=pltpu.CompilerParams(dimension_semantics=("arbitrary", "arbitrary"), vmem_limit_bytes=56 << 20),
        cost_estimate=pl.CostEstimate(flops=8 * tokens * SEQ * width * 4, bytes_accessed=100 << 20, transcendentals=0),
        name='attn_bwd',
    )(lengths, q, k, v, ctx, d_ctx, probs, cos_tab, sin_tab)


EPS = 1e-5
THETA = 10000.0
HIGH = 60 << 20


def whole(shape):
    return pl.BlockSpec(shape, lambda *i: (0,) * len(shape), pipeline_mode=pl.Buffered(1))


def part_of(shape, *at):
    return pl.BlockSpec(shape, lambda *i: at, pipeline_mode=pl.Buffered(1))


def partial(shape):
    return pl.BlockSpec(shape, lambda *i: (0,) * len(shape))


def rows_of(block, width):
    return pl.BlockSpec((block, width), lambda i: (i, 0))


def params(*semantics):
    return pltpu.CompilerParams(dimension_semantics=semantics or ('arbitrary',), vmem_limit_bytes=HIGH)


def cost(flops, moved):
    return pl.CostEstimate(flops=flops, bytes_accessed=moved, transcendentals=0)


def normal(x):
    mean = jnp.mean(x, axis=-1, keepdims=True)
    centered = x - mean
    inv = lax.rsqrt(jnp.mean(centered * centered, axis=-1, keepdims=True) + EPS)
    return centered * inv, inv


def norm_back(x, gain, grad):
    unit, inv = normal(x)
    scaled = grad * gain
    inner = scaled - jnp.mean(scaled, axis=-1, keepdims=True) - unit * jnp.mean(scaled * unit, axis=-1, keepdims=True)
    return inv * inner, unit


def eights(x):
    return jnp.sum(x.reshape(x.shape[0] // 8, 8, x.shape[1]), axis=0)


def qkv_kernel(x_ref, w_ref, b_ref, ln_ref, cos_ref, sin_ref, h_ref, q_ref, k_ref, v_ref):
    unit, _ = normal(x_ref[...].astype(jnp.float32))
    h_ref[...] = (unit * ln_ref[0:1] + ln_ref[1:2]).astype(jnp.bfloat16)
    for j, out_ref in enumerate((q_ref, k_ref, v_ref)):
        full = dot(h_ref[...], w_ref[j], NN) + b_ref[j:j + 1]
        if j == 2:
            out_ref[...] = full.astype(jnp.bfloat16)
            continue
        if j == 0:
            full = full * (HEAD_DIM ** -0.5)
        for c in range(0, full.shape[1], PAIR):
            out_ref[:, c:c + PAIR] = spin(full[:, c:c + PAIR], cos_ref[...], sin_ref[...], 1.0).astype(jnp.bfloat16)


def qkv(x, w, b, ln, cos, sin):
    tokens, width = x.shape
    block = 512
    row = rows_of(block, width)
    table = pl.BlockSpec((block, PAIR), lambda i: (i % (SEQ // block), 0))
    return pl.pallas_call(
        qkv_kernel, grid=(tokens // block,),
        in_specs=[row, part_of((3, width, width), 0, 0, 0), whole(b.shape), whole(ln.shape), table, table],
        out_specs=[row] * 4,
        out_shape=[jax.ShapeDtypeStruct(x.shape, jnp.bfloat16)] * 4,
        compiler_params=params(), cost_estimate=cost(6 * tokens * width * width, 26 << 20), name='qkv',
    )(x, w, b, ln, cos, sin)


def out_kernel(ctx_ref, x_ref, w_ref, b_ref, ln_ref, mid_ref, h_ref):
    mid = (x_ref[...].astype(jnp.float32) + dot(ctx_ref[...], w_ref[...], NN) + b_ref[3:4]).astype(jnp.bfloat16)
    mid_ref[...] = mid
    unit, _ = normal(mid.astype(jnp.float32))
    h_ref[...] = (unit * ln_ref[2:3] + ln_ref[3:4]).astype(jnp.bfloat16)


def out_proj(ctx, x, w, b, ln):
    tokens, width = x.shape
    block = 512
    row = rows_of(block, width)
    return pl.pallas_call(
        out_kernel, grid=(tokens // block,),
        in_specs=[row, row, part_of((None, width, width), 3, 0, 0), whole(b.shape), whole(ln.shape)], out_specs=[row] * 2,
        out_shape=[jax.ShapeDtypeStruct(x.shape, jnp.bfloat16)] * 2,
        compiler_params=params(), cost_estimate=cost(2 * tokens * width * width, 18 << 20), name='out_proj',
    )(ctx, x, w, b, ln)


def mlp_kernel(h_ref, mid_ref, wu_ref, bu_ref, wd_ref, bd_ref, act_ref, slope_ref, y_ref):
    total = mid_ref[...].astype(jnp.float32) + bd_ref[...]
    wide = wu_ref.shape[1]
    for c in range(0, wide, 1024):
        cols = slice(c, c + 1024)
        pre = dot(h_ref[...], wu_ref[:, cols], NN) + bu_ref[:, cols]
        cdf = 0.5 + 0.5 * lax.erf(pre * (1.0 / math.sqrt(2.0)))
        act_ref[:, cols] = (pre * cdf).astype(jnp.bfloat16)
        slope_ref[:, cols] = cdf + pre * (jnp.exp(-0.5 * pre * pre) * (1.0 / math.sqrt(2.0 * math.pi)))
        total = total + dot(act_ref[:, cols], wd_ref[cols], NN)
    y_ref[...] = total.astype(jnp.bfloat16)


def mlp(h, mid, wu, bu, wd, bd):
    tokens, width = h.shape
    wide = wu.shape[1]
    block = 256
    row, long = rows_of(block, width), rows_of(block, wide)
    return pl.pallas_call(
        mlp_kernel, grid=(tokens // block,),
        in_specs=[row, row, whole(wu.shape), whole(bu.shape), whole(wd.shape), whole(bd.shape)],
        out_specs=[long, long, row],
        out_shape=[jax.ShapeDtypeStruct((tokens, wide), jnp.bfloat16), jax.ShapeDtypeStruct((tokens, wide), jnp.float32),
                   jax.ShapeDtypeStruct(h.shape, jnp.bfloat16)],
        compiler_params=params(), cost_estimate=cost(4 * tokens * width * wide, 80 << 20), name='mlp',
    )(h, mid, wu, bu, wd, bd)


def mlp_back_kernel(dy_ref, slope_ref, wd_ref, wu_ref, mid_ref, ln_ref, wo_ref,
                    dpre_ref, dmid_ref, dctx_ref, gbu_ref, gln_ref):
    dy = dy_ref[...]
    grad = None
    wide = wu_ref.shape[1]
    first = pl.program_id(0) == 0

    @pl.when(first)
    def _():
        gbu_ref[...] = jnp.zeros_like(gbu_ref)
        gln_ref[...] = jnp.zeros_like(gln_ref)

    for c in range(0, wide, 1024):
        cols = slice(c, c + 1024)
        dpre = dot(dy, wd_ref[cols], NT) * slope_ref[:, cols]
        gbu_ref[:, cols] += eights(dpre)
        dpre_ref[:, cols] = dpre.astype(jnp.bfloat16)
        part = dot(dpre_ref[:, cols], wu_ref[:, cols], NT)
        grad = part if grad is None else grad + part
    dy = dy.astype(jnp.float32)
    back, unit = norm_back(mid_ref[...].astype(jnp.float32), ln_ref[2:3], grad)
    dmid = (dy + back).astype(jnp.bfloat16)
    dmid_ref[...] = dmid
    gln_ref[0:8] += eights(grad * unit)
    gln_ref[8:16] += eights(grad)
    gln_ref[16:24] += eights(dy)
    dctx_ref[...] = dot(dmid, wo_ref[...], NT).astype(jnp.bfloat16)


def mlp_back(dy, slope, wd, wu, mid, ln, wo):
    tokens, width = dy.shape
    wide = wu.shape[1]
    block = 256
    row, long = rows_of(block, width), rows_of(block, wide)
    half = jax.ShapeDtypeStruct(dy.shape, jnp.bfloat16)
    return pl.pallas_call(
        mlp_back_kernel, grid=(tokens // block,),
        in_specs=[row, long, whole(wd.shape), whole(wu.shape), row, whole(ln.shape), part_of((None, width, width), 3, 0, 0)],
        out_specs=[long, row, row, partial((8, wide)), partial((24, width))],
        out_shape=[jax.ShapeDtypeStruct((tokens, wide), jnp.bfloat16), half, half,
                   jax.ShapeDtypeStruct((8, wide), jnp.float32), jax.ShapeDtypeStruct((24, width), jnp.float32)],
        compiler_params=params(), cost_estimate=cost(2 * tokens * width * (2 * wide + width), 90 << 20), name='mlp_back',
    )(dy, slope, wd, wu, mid, ln, wo)


def in_back_kernel(dq_ref, dk_ref, dv_ref, w_ref, x_ref, ln_ref, dmid_ref, dx_ref, gln_ref):
    @pl.when(pl.program_id(0) == 0)
    def _():
        gln_ref[...] = jnp.zeros_like(gln_ref)

    grad = dot(dq_ref[...], w_ref[0], NT) + dot(dk_ref[...], w_ref[1], NT) + dot(dv_ref[...], w_ref[2], NT)
    back, unit = norm_back(x_ref[...].astype(jnp.float32), ln_ref[0:1], grad)
    dx_ref[...] = (dmid_ref[...].astype(jnp.float32) + back).astype(jnp.bfloat16)
    gln_ref[0:8] += eights(grad * unit)
    gln_ref[8:16] += eights(grad)


def in_back(dq, dk, dv, w, x, ln, dmid):
    tokens, width = x.shape
    block = 512
    row = rows_of(block, width)
    return pl.pallas_call(
        in_back_kernel, grid=(tokens // block,),
        in_specs=[row, row, row, part_of((3, width, width), 0, 0, 0), row, whole(ln.shape), row],
        out_specs=[row, partial((16, width))],
        out_shape=[jax.ShapeDtypeStruct(x.shape, jnp.bfloat16), jax.ShapeDtypeStruct((16, width), jnp.float32)],
        compiler_params=params(), cost_estimate=cost(6 * tokens * width * width, 34 << 20), name='in_back',
    )(dq, dk, dv, w, x, ln, dmid)


def share(grad, side, keep_ref, give_ref, at):
    low, high = grad
    keep_ref[at] = jnp.where(side == 0, low, high).astype(jnp.bfloat16)
    give_ref[at] = jnp.where(side == 0, high, low).astype(jnp.bfloat16)


def down_grad_kernel(side_ref, a_ref, b_ref, keep_ref, give_ref):
    grad = dot(a_ref[...], b_ref[...], TN)
    half = grad.shape[0] // 2
    share((grad[:half], grad[half:]), side_ref[0], keep_ref, give_ref, ...)


def down_grad(side, a, b):
    tokens, m = a.shape
    n = b.shape[1]
    chips = 8
    block = m // chips
    out = pl.BlockSpec((None, block // 2, n), lambda i, s: (i, 0, 0))
    return pl.pallas_call(
        down_grad_kernel,
        grid_spec=pltpu.PrefetchScalarGridSpec(
            num_scalar_prefetch=1, grid=(chips,),
            in_specs=[pl.BlockSpec((tokens, block), lambda i, s: (0, i)), whole(b.shape)], out_specs=[out, out]),
        out_shape=[jax.ShapeDtypeStruct((chips, block // 2, n), jnp.bfloat16)] * 2,
        compiler_params=params(), cost_estimate=cost(2 * tokens * m * n, 2 * (tokens * (m + n) + m * n)), name='down_grad',
    )(side, a, b)


def up_grad_kernel(side_ref, a_ref, b_ref, keep_ref, give_ref):
    grad = dot(a_ref[...], b_ref[...], TN)
    chips, half = keep_ref.shape[0], keep_ref.shape[1]
    for i in range(chips):
        r = 2 * i * half
        share((grad[r:r + half], grad[r + half:r + 2 * half]), side_ref[0], keep_ref, give_ref, i)


def up_grad(side, a, b):
    tokens, m = a.shape
    n = b.shape[1]
    chips, block = 8, 512
    out = pl.BlockSpec((chips, m // chips // 2, block), lambda i, s: (0, 0, i))
    return pl.pallas_call(
        up_grad_kernel,
        grid_spec=pltpu.PrefetchScalarGridSpec(
            num_scalar_prefetch=1, grid=(n // block,),
            in_specs=[whole(a.shape), pl.BlockSpec((tokens, block), lambda i, s: (0, i))], out_specs=[out, out]),
        out_shape=[jax.ShapeDtypeStruct((chips, m // chips // 2, n), jnp.bfloat16)] * 2,
        compiler_params=params(), cost_estimate=cost(2 * tokens * m * n, 2 * (tokens * (m + n) + m * n)), name='up_grad',
    )(side, a, b)


def attn_grad_kernel(side_ref, h_ref, ctx_ref, dq_ref, dk_ref, dv_ref, dmid_ref, keep_ref, give_ref, gb_ref):
    chips, half = keep_ref.shape[0], keep_ref.shape[2]
    for j, d_ref in enumerate((dq_ref, dk_ref, dv_ref, dmid_ref)):
        grad = dot((h_ref if j < 3 else ctx_ref)[...], d_ref[...], TN)
        for i in range(chips):
            r = 2 * i * half
            share((grad[r:r + half], grad[r + half:r + 2 * half]), side_ref[0], keep_ref, give_ref, (i, j))
        gb_ref[8 * j:8 * j + 8] = eights(d_ref[...].astype(jnp.float32))


def attn_grad(side, h, ctx, dq, dk, dv, dmid):
    tokens, width = h.shape
    chips, block = 8, 256
    cols = pl.BlockSpec((tokens, block), lambda i, s: (0, i))
    out = pl.BlockSpec((chips, 4, width // chips // 2, block), lambda i, s: (0, 0, 0, i))
    return pl.pallas_call(
        attn_grad_kernel,
        grid_spec=pltpu.PrefetchScalarGridSpec(
            num_scalar_prefetch=1, grid=(width // block,),
            in_specs=[whole(h.shape), whole(ctx.shape), cols, cols, cols, cols],
            out_specs=[out, out, pl.BlockSpec((32, block), lambda i, s: (0, i))]),
        out_shape=[jax.ShapeDtypeStruct((chips, 4, width // chips // 2, width), jnp.bfloat16)] * 2
        + [jax.ShapeDtypeStruct((32, width), jnp.float32)],
        compiler_params=params(), cost_estimate=cost(8 * tokens * width * width, 32 << 20), name='attn_grad',
    )(side, h, ctx, dq, dk, dv, dmid)


def rotary_tables():
    half = HEAD_DIM // 2
    inv_freq = 1.0 / (THETA ** (jnp.arange(half, dtype=jnp.float32) * (2.0 / HEAD_DIM)))
    angles = jnp.arange(SEQ, dtype=jnp.float32)[:, None] * inv_freq[None, :]
    cos, sin = jnp.cos(angles), jnp.sin(angles)
    return jnp.concatenate([cos] * 4, axis=1), jnp.concatenate([-sin, sin, -sin, sin], axis=1)


BITS = {'c': 1, 'x': 2, 'y': 4, 'z': 8}


def swap(value, axis_name, dim):
    return lax.ppermute(value, axis_name, [(i, i ^ BITS[dim]) for i in range(16)])


def bit_of(axis_name, dim):
    return (lax.axis_index(axis_name) // BITS[dim]) % 2


def gather_packed(packed, axis_name):
    held = packed[None]
    for dim in ('c', 'x', 'y', 'z'):
        got = swap(held, axis_name, dim)
        mine = bit_of(axis_name, dim)
        held = jnp.where(mine == 0, jnp.concatenate([held, got]), jnp.concatenate([got, held]))
    return held


def scatter_packed(full, axis_name):
    cur = full
    for dim in ('z', 'y', 'x', 'c'):
        mine = bit_of(axis_name, dim)
        half = cur.shape[0] // 2
        low, high = cur[:half], cur[half:]
        give = jnp.where(mine == 0, high, low)
        keep = jnp.where(mine == 0, low, high)
        cur = keep + swap(give, axis_name, dim)
    return cur[0]


def pack_params(b_attn, ln_par, b_up, b_down):
    layers = b_attn.shape[0]
    flat = jnp.concatenate([b_attn.reshape(layers, -1), ln_par.reshape(layers, -1), b_up, b_down], axis=1)
    return flat


def unpack_params(full, layer, n, nu):
    part = full[:, layer].astype(jnp.float32)
    b_attn = part[:, :4 * n].reshape(16, 4, n).transpose(1, 0, 2).reshape(4, 16 * n)
    ln = part[:, 4 * n:8 * n].reshape(16, 4, n).transpose(1, 0, 2).reshape(4, 16 * n)
    b_up = part[:, 8 * n:8 * n + nu].reshape(1, 16 * nu)
    b_down = part[:, 8 * n + nu:].reshape(1, 16 * n)
    return b_attn, ln, b_up, b_down


def solution(mesh):
    axis_name = mesh.axis_names[0]
    batch_spec = P(axis_name)
    weight_specs = (P(None, None, axis_name, None), P(None, None, axis_name), P(None, None, axis_name),
                    P(None, axis_name, None), P(None, axis_name), P(None, axis_name, None), P(None, axis_name))

    def device_step(x, lengths, d_y, w_attn, b_attn, ln_par, w_up, b_up, w_down, b_down):
        layers = w_attn.shape[0]
        seqs, seq_len, width = x.shape
        tokens = seqs * seq_len
        n, nu = b_attn.shape[2], b_up.shape[1]
        cos, sin = rotary_tables()
        gather = functools.partial(lax.all_gather, axis_name=axis_name, tiled=True)
        side = bit_of(axis_name, 'c').reshape(1)
        after = lax.optimization_barrier

        def join(keep, got):
            return (keep.astype(jnp.float32) + got.astype(jnp.float32)).astype(jnp.bfloat16)

        def spread_out(pair):
            groups = [[2 * i + c for i in range(8)] for c in range(2)]
            return lax.all_to_all(pair, axis_name, split_axis=0, concat_axis=0, axis_index_groups=groups, tiled=True)

        def total(parts):
            return jnp.sum(parts.astype(jnp.float32), axis=0)

        small = gather_packed(pack_params(b_attn, ln_par, b_up, b_down), axis_name)
        hidden = x.reshape(tokens, width)
        saved = []
        for l in range(layers):
            ba, ln, bu, bd = unpack_params(small, l, n, nu)
            wa = gather(w_attn[l], axis=1)
            wu = gather(w_up[l], axis=0)
            wd = gather(w_down[l], axis=0)
            h_one, q, k, v = qkv(hidden, wa, ba, ln, cos, sin)
            ctx, probs = attn_fwd(lengths, q, k, v)
            mid, h_two = out_proj(ctx, hidden, wa, ba, ln)
            act, slope, out = mlp(h_two, mid, wu, bu, wd, bd)
            saved.append((hidden, h_one, q, k, v, ctx, probs, mid, h_two, act, slope, wa, wu, wd, ln))
            hidden = out
        grad = d_y.reshape(tokens, width)
        grads = [None] * layers
        for l in reversed(range(layers)):
            if l + 1 < layers:
                flying = spread_out(pair)
            x_in, h_one, q, k, v, ctx, probs, mid, h_two, act, slope, wa, wu, wd, ln = saved[l]
            keep, give = down_grad(side, act, grad)
            give, grad = after((give, grad))
            got = swap(give, axis_name, 'c')
            d_pre, d_mid, d_ctx, gb_up, gln_two = mlp_back(grad, slope, wd, wu, mid, ln, wa)
            got, d_pre = after((got, d_pre))
            if l + 1 < layers:
                flying, d_pre = after((flying, d_pre))
                grads[l + 1][0] = total(flying)
            pair, d_pre = after((join(keep, got), d_pre))
            flying = spread_out(pair)
            keep, give = up_grad(side, h_two, d_pre)
            give, d_ctx = after((give, d_ctx))
            got = swap(give, axis_name, 'c')
            dq, dk, dv = attn_bwd(lengths, q, k, v, ctx, d_ctx, probs, cos, sin)
            flying, got, dq = after((flying, got, dq))
            g_down = total(flying)
            pair, dq = after((join(keep, got), dq))
            flying = spread_out(pair)
            keep, give, gb_attn = attn_grad(side, h_one, ctx, dq, dk, dv, d_mid)
            give, dq = after((give, dq))
            got = swap(give, axis_name, 'c')
            if l > 0:
                grad, gln_one = in_back(dq, dk, dv, wa, x_in, ln, d_mid)
                flying, got, grad = after((flying, got, grad))
                g_up = total(flying)
                pair, grad = after((join(keep, got), grad))
            else:
                flying, got, dq = after((flying, got, dq))
                g_up = total(flying)
                pair, dq = after((join(keep, got), dq))
                flying = spread_out(pair)
                grad, gln_one = in_back(dq, dk, dv, wa, x_in, ln, d_mid)
            sums_two = jnp.sum(gln_two.reshape(3, 8, width), axis=1)
            sums_one = jnp.sum(gln_one.reshape(2, 8, width), axis=1)
            gb_four = jnp.sum(gb_attn.reshape(4, 8, width), axis=1)
            gb_wide = jnp.sum(gb_up, axis=0)
            by_dev = lambda s: s.reshape(-1, 16, n).transpose(1, 0, 2).reshape(16, -1)
            packed = jnp.concatenate([by_dev(gb_four), by_dev(sums_one), by_dev(sums_two[:2]),
                                      gb_wide.reshape(16, nu), by_dev(sums_two[2:3])], axis=1)
            grads[l] = [None, g_up, g_down, packed]
        got = scatter_packed(jnp.stack([g[3] for g in grads], axis=1), axis_name)
        grads[0][0] = total(flying)
        g_attn, g_up, g_down = (jnp.stack([g[i] for g in grads]) for i in range(3))
        return (grad.reshape(x.shape), g_attn, got[:, :4 * n].reshape(layers, 4, n), got[:, 4 * n:8 * n].reshape(layers, 4, n),
                g_up, got[:, 8 * n:8 * n + nu], g_down, got[:, 8 * n + nu:])

    return jax.shard_map(device_step, mesh=mesh,
                         in_specs=(batch_spec, batch_spec, batch_spec) + weight_specs,
                         out_specs=(batch_spec,) + weight_specs,
                         check_vma=False)
```

```python
import functools, math
import jax
import jax.numpy as jnp
from jax import lax
from jax.experimental import pallas as pl
from jax.experimental.pallas import tpu as pltpu
from jax.sharding import PartitionSpec as P

HEAD_DIM = 64
SEQ = 1024
QT = 256
RB = 64
PAIR = 2 * HEAD_DIM
NEG_BIG = -1e30
NN = (((1,), (0,)), ((), ()))
NT = (((1,), (1,)), ((), ()))
TN = (((0,), (0,)), ((), ()))


def dot(a, b, dims):
    return lax.dot_general(a, b, dims, preferred_element_type=jnp.float32)


def lane_iota(rows):
    return lax.broadcasted_iota(jnp.int32, (rows, PAIR), 1)


def attn_fwd_kernel(len_ref, q_ref, k_ref, v_ref, ctx_ref, p_ref, ka_ref, qa_ref, vt_ref, e_ref, top_ref, sum_ref, ctxt_ref):
    seq_len = len_ref[pl.program_id(0)]
    lane = lane_iota(1)
    hidden_key = lax.broadcasted_iota(jnp.int32, (SEQ, PAIR), 0) >= seq_len
    for h in range(2):
        mine = (lane // HEAD_DIM) == h
        aux = lane == (1 - h) * HEAD_DIM
        own = mine.astype(jnp.float32).astype(jnp.bfloat16)
        one = aux.astype(jnp.float32).astype(jnp.bfloat16)
        bar = jnp.where(aux, NEG_BIG, 0.0).astype(jnp.bfloat16)
        ka_ref[h] = jnp.where(hidden_key, jnp.broadcast_to(bar, (SEQ, PAIR)), k_ref[...] * own)
        qa_ref[h] = q_ref[...] * own + one
    vt_ref[...] = v_ref[...].T

    def at(t):
        return pl.ds(pl.multiple_of(t * QT, QT), QT)

    def fold(x, op):
        while x.shape[0] > 8:
            half = x.shape[0] // 2
            x = op(x[:half], x[half:])
        return x

    def spread(x):
        return jnp.concatenate([x] * (RB // 8), axis=0)

    def rise(t, h):
        s = dot(ka_ref[h], qa_ref[h, at(t)], NT)
        for c in range(SEQ // RB):
            part = s[c * RB:(c + 1) * RB]
            top = fold(part, jnp.maximum)
            e = jnp.exp(part - spread(top))
            e_ref[h, c * RB:(c + 1) * RB] = e
            top_ref[h, c * 8:(c + 1) * 8] = top
            sum_ref[h, c * 8:(c + 1) * 8] = fold(e, jnp.add)

    def settle(t, h):
        tops = top_ref[h]
        weight = jnp.exp(tops - jnp.max(tops, axis=0, keepdims=True))
        scale = weight * (1.0 / jnp.sum(weight * sum_ref[h], axis=0, keepdims=True))
        for c in range(SEQ // RB):
            p_ref[h, c * RB:(c + 1) * RB, at(t)] = (e_ref[h, c * RB:(c + 1) * RB] * spread(scale[c * 8:(c + 1) * 8])).astype(jnp.bfloat16)
        rows = slice(h * HEAD_DIM, (h + 1) * HEAD_DIM)
        ctxt_ref[rows, at(t)] = dot(vt_ref[rows], p_ref[h, :, at(t)], NN)

    last = SEQ // QT - 1
    rise(0, 0)

    def turn(t, _):
        settle(t, 0)
        rise(t, 1)
        rise(jnp.minimum(t + 1, last), 0)
        settle(t, 1)
        return 0

    lax.fori_loop(0, SEQ // QT, turn, 0)
    ctx_ref[...] = ctxt_ref[...].T.astype(jnp.bfloat16)


def attn_fwd(lengths, q, k, v):
    tokens, width = q.shape
    seqs, pairs = tokens // SEQ, width // PAIR
    spec = pl.BlockSpec((SEQ, PAIR), lambda b, h, n: (b, h))
    return pl.pallas_call(
        attn_fwd_kernel,
        grid_spec=pltpu.PrefetchScalarGridSpec(
            num_scalar_prefetch=1, grid=(seqs, pairs),
            in_specs=[spec, spec, spec],
            out_specs=[spec, pl.BlockSpec((None, 2, SEQ, SEQ), lambda b, h, n: (b, h, 0, 0))],
            scratch_shapes=[pltpu.VMEM((2, SEQ, PAIR), jnp.bfloat16), pltpu.VMEM((2, SEQ, PAIR), jnp.bfloat16),
                            pltpu.VMEM((PAIR, SEQ), jnp.bfloat16), pltpu.VMEM((2, SEQ, QT), jnp.float32), pltpu.VMEM((2, SEQ // RB * 8, QT), jnp.float32), pltpu.VMEM((2, SEQ // RB * 8, QT), jnp.float32),
                            pltpu.VMEM((PAIR, SEQ), jnp.float32)]),
        out_shape=[jax.ShapeDtypeStruct((tokens, width), jnp.bfloat16),
                   jax.ShapeDtypeStruct((seqs, 2 * pairs, SEQ, SEQ), jnp.bfloat16)],
        compiler_params=pltpu.CompilerParams(dimension_semantics=("arbitrary", "arbitrary"), vmem_limit_bytes=56 << 20),
        cost_estimate=pl.CostEstimate(flops=4 * tokens * SEQ * width * 4, bytes_accessed=90 << 20, transcendentals=tokens * SEQ * 16),
        name='attn_fwd',
    )(lengths, q, k, v)


def spin(x, cos, sin, sign):
    half = HEAD_DIM // 2
    low = (lax.broadcasted_iota(jnp.int32, x.shape, 1) % HEAD_DIM) < half
    other = jnp.where(low, pltpu.roll(x, PAIR - half, 1), pltpu.roll(x, half, 1))
    return x * cos + other * (sin * sign)


def attn_bwd_kernel(axis, units, last, q_ref, k_ref, v_ref, o_ref, do_ref, p_ref, cos_ref, sin_ref, *refs):
    pairs, (dq_ref, dk_ref, dv_ref), lands = refs[:units], refs[units:units + 3], refs[units + 3:2 * units + 3]
    doh_ref, qh_ref, kt_ref, d_ref, ds_ref, dqt_ref, *sems = refs[2 * units + 3:]
    ride(axis, last, pl.program_id(0) * pl.num_programs(1) + pl.program_id(1), pairs, lands, *sems)
    lane = lane_iota(1)
    for h in range(2):
        own = ((lane // HEAD_DIM) == h).astype(jnp.float32).astype(jnp.bfloat16)
        doh_ref[h] = do_ref[...] * own
        qh_ref[h] = q_ref[...] * own
    kt_ref[...] = k_ref[...].T
    prod = (do_ref[...].astype(jnp.float32) * o_ref[...].astype(jnp.float32)).T
    for h in range(2):
        d_ref[h:h + 1] = jnp.sum(prod[h * HEAD_DIM:(h + 1) * HEAD_DIM], axis=0, keepdims=True)
    for h in range(2):
        for t in range(SEQ // QT):
            cols = slice(t * QT, (t + 1) * QT)
            dp = dot(v_ref[...], doh_ref[h, cols], NT)
            ds_ref[h, :, cols] = (p_ref[h, :, cols].astype(jnp.float32) * (dp - d_ref[h:h + 1, cols])).astype(jnp.bfloat16)
    dv_ref[...] = (dot(p_ref[0], doh_ref[0], NN) + dot(p_ref[1], doh_ref[1], NN)).astype(jnp.bfloat16)
    for h in range(2):
        dqt_ref[h * HEAD_DIM:(h + 1) * HEAD_DIM] = dot(kt_ref[h * HEAD_DIM:(h + 1) * HEAD_DIM], ds_ref[h], NN)
    dk = dot(ds_ref[0], qh_ref[0], NN) + dot(ds_ref[1], qh_ref[1], NN)
    dk_ref[...] = spin(dk, cos_ref[...], sin_ref[...], -1.0).astype(jnp.bfloat16)
    dq_ref[...] = (spin(dqt_ref[...].T, cos_ref[...], sin_ref[...], -1.0) * (HEAD_DIM ** -0.5)).astype(jnp.bfloat16)


def attn_bwd(axis, number, units, q, k, v, ctx, d_ctx, probs, cos_tab, sin_tab):
    tokens, width = q.shape
    seqs, pairs = tokens // SEQ, width // PAIR
    spec = pl.BlockSpec((SEQ, PAIR), lambda b, h: (b, h))
    table = pl.BlockSpec((SEQ, PAIR), lambda b, h: (0, 0))
    return pl.pallas_call(
        functools.partial(attn_bwd_kernel, axis, len(units), seqs * pairs - 1), grid=(seqs, pairs),
        in_specs=[spec] * 5 + [pl.BlockSpec((None, 2, SEQ, SEQ), lambda b, h: (b, h, 0, 0)), table, table] + ride_specs(units),
        out_specs=[spec] * 3 + ride_specs(units),
        scratch_shapes=[pltpu.VMEM((2, SEQ, PAIR), jnp.bfloat16), pltpu.VMEM((2, SEQ, PAIR), jnp.bfloat16),
                        pltpu.VMEM((PAIR, SEQ), jnp.bfloat16), pltpu.VMEM((8, SEQ), jnp.float32),
                        pltpu.VMEM((2, SEQ, SEQ), jnp.bfloat16), pltpu.VMEM((PAIR, SEQ), jnp.float32)] + ride_scratch(len(units)),
        out_shape=[jax.ShapeDtypeStruct((tokens, width), jnp.bfloat16)] * 3 + same(units),
        compiler_params=ride_params(number, 'arbitrary', 'arbitrary'),
        cost_estimate=pl.CostEstimate(flops=8 * tokens * SEQ * width * 4, bytes_accessed=100 << 20, transcendentals=0),
        name='attn_bwd',
    )(q, k, v, ctx, d_ctx, probs, cos_tab, sin_tab, *units)


EPS = 1e-5
THETA = 10000.0
HIGH = 60 << 20


def whole(shape):
    return pl.BlockSpec(shape, lambda *i: (0,) * len(shape), pipeline_mode=pl.Buffered(1))


def part_of(shape, *at):
    return pl.BlockSpec(shape, lambda *i: at, pipeline_mode=pl.Buffered(1))


def partial(shape):
    return pl.BlockSpec(shape, lambda *i: (0,) * len(shape))


def rows_of(block, width):
    return pl.BlockSpec((block, width), lambda i: (i, 0))


def params(*semantics):
    return pltpu.CompilerParams(dimension_semantics=semantics or ('arbitrary',), vmem_limit_bytes=HIGH)


def cost(flops, moved):
    return pl.CostEstimate(flops=flops, bytes_accessed=moved, transcendentals=0)


def normal(x):
    mean = jnp.mean(x, axis=-1, keepdims=True)
    centered = x - mean
    inv = lax.rsqrt(jnp.mean(centered * centered, axis=-1, keepdims=True) + EPS)
    return centered * inv, inv


def norm_back(x, gain, grad):
    unit, inv = normal(x)
    scaled = grad * gain
    inner = scaled - jnp.mean(scaled, axis=-1, keepdims=True) - unit * jnp.mean(scaled * unit, axis=-1, keepdims=True)
    return inv * inner, unit


def eights(x):
    return jnp.sum(x.reshape(x.shape[0] // 8, 8, x.shape[1]), axis=0)


def ride(axis, last, step, pairs, lands, send_sem, recv_sem, own_sem):
    me = lax.axis_index(axis)
    side, chip = me % 2, me // 2
    chips = pairs[0].shape[0]

    def peer(j):
        return ((chip + j) % chips) * 2 + side

    def copies():
        made = []
        for u, (pair, land) in enumerate(zip(pairs, lands)):
            for j in range(1, chips):
                made.append(pltpu.make_async_remote_copy(
                    src_ref=pair.at[(chip + j) % chips], dst_ref=land.at[chip], send_sem=send_sem.at[u, j], recv_sem=recv_sem.at[u, j],
                    device_id=(peer(j),), device_id_type=MESH))
            made.append(pltpu.make_async_copy(pair.at[chip], land.at[chip], own_sem.at[u]))
        return made

    @pl.when(step == 0)
    def _():
        barrier = pltpu.get_barrier_semaphore()
        for j in range(1, chips):
            pl.semaphore_signal(barrier, inc=1, device_id=(peer(j),), device_id_type=MESH)

    @pl.when(step == 1)
    def _():
        pl.semaphore_wait(pltpu.get_barrier_semaphore(), chips - 1)
        for c in copies():
            c.start()

    @pl.when(step == last)
    def _():
        for c in copies():
            c.wait()


MESH = pl.DeviceIdType.MESH


def ride_scratch(units):
    return [pltpu.SemaphoreType.DMA((units, 8)), pltpu.SemaphoreType.DMA((units, 8)), pltpu.SemaphoreType.DMA((units,))]


def ride_specs(pairs):
    return [pl.BlockSpec(memory_space=pl.ANY)] * len(pairs)


def same(pairs):
    return [jax.ShapeDtypeStruct(p.shape, p.dtype) for p in pairs]


def ride_params(number, *semantics):
    return pltpu.CompilerParams(dimension_semantics=semantics or ('arbitrary',), vmem_limit_bytes=HIGH, collective_id=number, has_side_effects=True)


def qkv_kernel(x_ref, w_ref, b_ref, ln_ref, cos_ref, sin_ref, h_ref, q_ref, k_ref, v_ref):
    unit, _ = normal(x_ref[...].astype(jnp.float32))
    h_ref[...] = (unit * ln_ref[0:1] + ln_ref[1:2]).astype(jnp.bfloat16)
    for j, out_ref in enumerate((q_ref, k_ref, v_ref)):
        full = dot(h_ref[...], w_ref[j], NN) + b_ref[j:j + 1]
        if j == 2:
            out_ref[...] = full.astype(jnp.bfloat16)
            continue
        if j == 0:
            full = full * (HEAD_DIM ** -0.5)
        for c in range(0, full.shape[1], PAIR):
            out_ref[:, c:c + PAIR] = spin(full[:, c:c + PAIR], cos_ref[...], sin_ref[...], 1.0).astype(jnp.bfloat16)


def qkv(x, w, b, ln, cos, sin):
    tokens, width = x.shape
    block = 512
    row = rows_of(block, width)
    table = pl.BlockSpec((block, PAIR), lambda i: (i % (SEQ // block), 0))
    return pl.pallas_call(
        qkv_kernel, grid=(tokens // block,),
        in_specs=[row, part_of((3, width, width), 0, 0, 0), whole(b.shape), whole(ln.shape), table, table],
        out_specs=[row] * 4,
        out_shape=[jax.ShapeDtypeStruct(x.shape, jnp.bfloat16)] * 4,
        compiler_params=params(), cost_estimate=cost(6 * tokens * width * width, 26 << 20), name='qkv',
    )(x, w, b, ln, cos, sin)


def out_kernel(ctx_ref, x_ref, w_ref, b_ref, ln_ref, mid_ref, h_ref):
    mid = (x_ref[...].astype(jnp.float32) + dot(ctx_ref[...], w_ref[...], NN) + b_ref[3:4]).astype(jnp.bfloat16)
    mid_ref[...] = mid
    unit, _ = normal(mid.astype(jnp.float32))
    h_ref[...] = (unit * ln_ref[2:3] + ln_ref[3:4]).astype(jnp.bfloat16)


def out_proj(ctx, x, w, b, ln):
    tokens, width = x.shape
    block = 512
    row = rows_of(block, width)
    return pl.pallas_call(
        out_kernel, grid=(tokens // block,),
        in_specs=[row, row, part_of((None, width, width), 3, 0, 0), whole(b.shape), whole(ln.shape)], out_specs=[row] * 2,
        out_shape=[jax.ShapeDtypeStruct(x.shape, jnp.bfloat16)] * 2,
        compiler_params=params(), cost_estimate=cost(2 * tokens * width * width, 18 << 20), name='out_proj',
    )(ctx, x, w, b, ln)


def mlp_kernel(h_ref, mid_ref, wu_ref, bu_ref, wd_ref, bd_ref, act_ref, slope_ref, y_ref):
    total = mid_ref[...].astype(jnp.float32) + bd_ref[...]
    wide = wu_ref.shape[1]
    for c in range(0, wide, 1024):
        cols = slice(c, c + 1024)
        pre = dot(h_ref[...], wu_ref[:, cols], NN) + bu_ref[:, cols]
        cdf = 0.5 + 0.5 * lax.erf(pre * (1.0 / math.sqrt(2.0)))
        act_ref[:, cols] = (pre * cdf).astype(jnp.bfloat16)
        slope_ref[:, cols] = cdf + pre * (jnp.exp(-0.5 * pre * pre) * (1.0 / math.sqrt(2.0 * math.pi)))
        total = total + dot(act_ref[:, cols], wd_ref[cols], NN)
    y_ref[...] = total.astype(jnp.bfloat16)


def mlp(h, mid, wu, bu, wd, bd):
    tokens, width = h.shape
    wide = wu.shape[1]
    block = 256
    row, long = rows_of(block, width), rows_of(block, wide)
    return pl.pallas_call(
        mlp_kernel, grid=(tokens // block,),
        in_specs=[row, row, whole(wu.shape), whole(bu.shape), whole(wd.shape), whole(bd.shape)],
        out_specs=[long, long, row],
        out_shape=[jax.ShapeDtypeStruct((tokens, wide), jnp.bfloat16), jax.ShapeDtypeStruct((tokens, wide), jnp.float32),
                   jax.ShapeDtypeStruct(h.shape, jnp.bfloat16)],
        compiler_params=params(), cost_estimate=cost(4 * tokens * width * wide, 80 << 20), name='mlp',
    )(h, mid, wu, bu, wd, bd)


def mlp_back_kernel(axis, units, last, dy_ref, slope_ref, wd_ref, wu_ref, mid_ref, ln_ref, wo_ref, *refs):
    pairs, (dpre_ref, dmid_ref, dctx_ref, gbu_ref, gln_ref), lands, sems = refs[:units], refs[units:units + 5], refs[units + 5:2 * units + 5], refs[2 * units + 5:]
    ride(axis, last, pl.program_id(0), pairs, lands, *sems)
    dy = dy_ref[...]
    grad = None
    wide = wu_ref.shape[1]
    first = pl.program_id(0) == 0

    @pl.when(first)
    def _():
        gbu_ref[...] = jnp.zeros_like(gbu_ref)
        gln_ref[...] = jnp.zeros_like(gln_ref)

    for c in range(0, wide, 1024):
        cols = slice(c, c + 1024)
        dpre = dot(dy, wd_ref[cols], NT) * slope_ref[:, cols]
        gbu_ref[:, cols] += eights(dpre)
        dpre_ref[:, cols] = dpre.astype(jnp.bfloat16)
        part = dot(dpre_ref[:, cols], wu_ref[:, cols], NT)
        grad = part if grad is None else grad + part
    dy = dy.astype(jnp.float32)
    back, unit = norm_back(mid_ref[...].astype(jnp.float32), ln_ref[2:3], grad)
    dmid = (dy + back).astype(jnp.bfloat16)
    dmid_ref[...] = dmid
    gln_ref[0:8] += eights(grad * unit)
    gln_ref[8:16] += eights(grad)
    gln_ref[16:24] += eights(dy)
    dctx_ref[...] = dot(dmid, wo_ref[...], NT).astype(jnp.bfloat16)


def mlp_back(axis, number, pairs, dy, slope, wd, wu, mid, ln, wo):
    tokens, width = dy.shape
    wide = wu.shape[1]
    block = 256
    row, long = rows_of(block, width), rows_of(block, wide)
    half = jax.ShapeDtypeStruct(dy.shape, jnp.bfloat16)
    return pl.pallas_call(
        functools.partial(mlp_back_kernel, axis, len(pairs), tokens // block - 1), grid=(tokens // block,),
        in_specs=[row, long, whole(wd.shape), whole(wu.shape), row, whole(ln.shape), part_of((None, width, width), 3, 0, 0)] + ride_specs(pairs),
        out_specs=[long, row, row, partial((8, wide)), partial((24, width))] + ride_specs(pairs),
        out_shape=[jax.ShapeDtypeStruct((tokens, wide), jnp.bfloat16), half, half,
                   jax.ShapeDtypeStruct((8, wide), jnp.float32), jax.ShapeDtypeStruct((24, width), jnp.float32)] + same(pairs),
        scratch_shapes=ride_scratch(len(pairs)),
        compiler_params=ride_params(number), cost_estimate=cost(2 * tokens * width * (2 * wide + width), 90 << 20), name='mlp_back',
    )(dy, slope, wd, wu, mid, ln, wo, *pairs)


def in_back_kernel(axis, units, last, dq_ref, dk_ref, dv_ref, w_ref, x_ref, ln_ref, dmid_ref, *refs):
    pairs, (dx_ref, gln_ref), lands, sems = refs[:units], refs[units:units + 2], refs[units + 2:2 * units + 2], refs[2 * units + 2:]
    if units:
        ride(axis, last, pl.program_id(0), pairs, lands, *sems)

    @pl.when(pl.program_id(0) == 0)
    def _():
        gln_ref[...] = jnp.zeros_like(gln_ref)

    grad = dot(dq_ref[...], w_ref[0], NT) + dot(dk_ref[...], w_ref[1], NT) + dot(dv_ref[...], w_ref[2], NT)
    back, unit = norm_back(x_ref[...].astype(jnp.float32), ln_ref[0:1], grad)
    dx_ref[...] = (dmid_ref[...].astype(jnp.float32) + back).astype(jnp.bfloat16)
    gln_ref[0:8] += eights(grad * unit)
    gln_ref[8:16] += eights(grad)


def in_back(axis, number, pairs, dq, dk, dv, w, x, ln, dmid):
    tokens, width = x.shape
    block = 512
    row = rows_of(block, width)
    return pl.pallas_call(
        functools.partial(in_back_kernel, axis, len(pairs), tokens // block - 1), grid=(tokens // block,),
        in_specs=[row, row, row, part_of((3, width, width), 0, 0, 0), row, whole(ln.shape), row] + ride_specs(pairs),
        out_specs=[row, partial((16, width))] + ride_specs(pairs),
        out_shape=[jax.ShapeDtypeStruct(x.shape, jnp.bfloat16), jax.ShapeDtypeStruct((16, width), jnp.float32)] + same(pairs),
        scratch_shapes=ride_scratch(len(pairs)) if pairs else [],
        compiler_params=ride_params(number) if pairs else params(), cost_estimate=cost(6 * tokens * width * width, 34 << 20), name='in_back',
    )(dq, dk, dv, w, x, ln, dmid, *pairs)


def swap_step(axis, steps, make, keep_ref, send_ref, recv_ref, send_sem, recv_sem, out_ref):
    i = pl.program_id(0)
    me = lax.axis_index(axis)
    side = me % 2
    other = me + 1 - 2 * side

    def copy(j):
        return pltpu.make_async_remote_copy(
            src_ref=send_ref.at[j], dst_ref=recv_ref.at[j], send_sem=send_sem.at[j], recv_sem=recv_sem.at[j],
            device_id=(other,), device_id_type=MESH)

    def put(at, low, high):
        keep_ref[(i % 3,) + at] = jnp.where(side == 0, low, high)
        send_ref[(i,) + at] = jnp.where(side == 0, high, low).astype(jnp.bfloat16)

    def finish():
        out_ref[...] = (keep_ref[(i + 1) % 3] + recv_ref[i - 2].astype(jnp.float32)).astype(jnp.bfloat16)

    @pl.when(i == 0)
    def _():
        barrier = pltpu.get_barrier_semaphore()
        pl.semaphore_signal(barrier, inc=1, device_id=(other,), device_id_type=MESH)
        pl.semaphore_wait(barrier, 1)

    @pl.when((i >= 1) & (i <= steps))
    def _():
        copy(i - 1).start()

    @pl.when(i >= 2)
    def _():
        copy(i - 2).wait()

    @pl.when(i < 2)
    def _():
        make(put)

    @pl.when((i >= 2) & (i < steps))
    def _():
        make(put)
        finish()

    @pl.when(i >= steps)
    def _():
        finish()


def swap_scratch(steps, block):
    return [pltpu.VMEM((3,) + block, jnp.float32), pltpu.VMEM((steps,) + block, jnp.bfloat16), pltpu.VMEM((steps,) + block, jnp.bfloat16),
            pltpu.SemaphoreType.DMA((steps,)), pltpu.SemaphoreType.DMA((steps,))]


def swap_params(number):
    return pltpu.CompilerParams(dimension_semantics=('arbitrary',), vmem_limit_bytes=HIGH, collective_id=number, has_side_effects=True)


def down_grad_kernel(axis, steps, a_ref, b_ref, out_ref, *scratch):
    def make(put):
        grad = dot(a_ref[...], b_ref[...], TN)
        half = grad.shape[0] // 2
        put((), grad[:half], grad[half:])

    swap_step(axis, steps, make, *scratch, out_ref)


def down_grad(axis, number, a, b):
    tokens, m = a.shape
    n = b.shape[1]
    chips = 8
    block = m // chips
    return pl.pallas_call(
        functools.partial(down_grad_kernel, axis, chips), grid=(chips + 2,),
        in_specs=[pl.BlockSpec((tokens, block), lambda i: (0, jnp.minimum(i, chips - 1))), whole(b.shape)],
        out_specs=pl.BlockSpec((None, block // 2, n), lambda i: (jnp.maximum(i - 2, 0), 0, 0)),
        out_shape=jax.ShapeDtypeStruct((chips, block // 2, n), jnp.bfloat16),
        scratch_shapes=swap_scratch(chips, (block // 2, n)),
        compiler_params=swap_params(number), cost_estimate=cost(2 * tokens * m * n, 2 * (tokens * (m + n) + m * n)), name='down_grad',
    )(a, b)


def up_grad_kernel(axis, steps, a_ref, b_ref, out_ref, *scratch):
    def make(put):
        grad = dot(a_ref[...], b_ref[...], TN)
        chips, half = out_ref.shape[0], out_ref.shape[1]
        for c in range(chips):
            r = 2 * c * half
            put((c,), grad[r:r + half], grad[r + half:r + 2 * half])

    swap_step(axis, steps, make, *scratch, out_ref)


def up_grad(axis, number, a, b):
    tokens, m = a.shape
    n = b.shape[1]
    chips, block = 8, 512
    steps = n // block
    half = m // chips // 2
    return pl.pallas_call(
        functools.partial(up_grad_kernel, axis, steps), grid=(steps + 2,),
        in_specs=[whole(a.shape), pl.BlockSpec((tokens, block), lambda i: (0, jnp.minimum(i, steps - 1)))],
        out_specs=pl.BlockSpec((chips, half, block), lambda i: (0, 0, jnp.maximum(i - 2, 0))),
        out_shape=jax.ShapeDtypeStruct((chips, half, n), jnp.bfloat16),
        scratch_shapes=swap_scratch(steps, (chips, half, block)),
        compiler_params=swap_params(number), cost_estimate=cost(2 * tokens * m * n, 2 * (tokens * (m + n) + m * n)), name='up_grad',
    )(a, b)


def attn_grad_kernel(axis, steps, h_ref, ctx_ref, dq_ref, dk_ref, dv_ref, dmid_ref, out_ref, gb_ref, *scratch):
    def make(put):
        chips, half = out_ref.shape[0], out_ref.shape[2]
        for j, d_ref in enumerate((dq_ref, dk_ref, dv_ref, dmid_ref)):
            grad = dot((h_ref if j < 3 else ctx_ref)[...], d_ref[...], TN)
            for c in range(chips):
                r = 2 * c * half
                put((c, j), grad[r:r + half], grad[r + half:r + 2 * half])
            gb_ref[8 * j:8 * j + 8] = eights(d_ref[...].astype(jnp.float32))

    swap_step(axis, steps, make, *scratch, out_ref)


def attn_grad(axis, number, h, ctx, dq, dk, dv, dmid):
    tokens, width = h.shape
    chips, block = 8, 256
    steps = width // block
    half = width // chips // 2
    cols = pl.BlockSpec((tokens, block), lambda i: (0, jnp.minimum(i, steps - 1)))
    return pl.pallas_call(
        functools.partial(attn_grad_kernel, axis, steps), grid=(steps + 2,),
        in_specs=[whole(h.shape), whole(ctx.shape), cols, cols, cols, cols],
        out_specs=[pl.BlockSpec((chips, 4, half, block), lambda i: (0, 0, 0, jnp.maximum(i - 2, 0))),
                   pl.BlockSpec((32, block), lambda i: (0, jnp.minimum(i, steps - 1)))],
        out_shape=[jax.ShapeDtypeStruct((chips, 4, half, width), jnp.bfloat16), jax.ShapeDtypeStruct((32, width), jnp.float32)],
        scratch_shapes=swap_scratch(steps, (chips, 4, half, block)),
        compiler_params=swap_params(number), cost_estimate=cost(8 * tokens * width * width, 32 << 20), name='attn_grad',
    )(h, ctx, dq, dk, dv, dmid)


def rotary_tables():
    half = HEAD_DIM // 2
    inv_freq = 1.0 / (THETA ** (jnp.arange(half, dtype=jnp.float32) * (2.0 / HEAD_DIM)))
    angles = jnp.arange(SEQ, dtype=jnp.float32)[:, None] * inv_freq[None, :]
    cos, sin = jnp.cos(angles), jnp.sin(angles)
    return jnp.concatenate([cos] * 4, axis=1), jnp.concatenate([-sin, sin, -sin, sin], axis=1)


BITS = {'c': 1, 'x': 2, 'y': 4, 'z': 8}


def swap(value, axis_name, dim):
    return lax.ppermute(value, axis_name, [(i, i ^ BITS[dim]) for i in range(16)])


def bit_of(axis_name, dim):
    return (lax.axis_index(axis_name) // BITS[dim]) % 2


def gather_packed(packed, axis_name):
    held = packed[None]
    for dim in ('c', 'x', 'y', 'z'):
        got = swap(held, axis_name, dim)
        mine = bit_of(axis_name, dim)
        held = jnp.where(mine == 0, jnp.concatenate([held, got]), jnp.concatenate([got, held]))
    return held


def scatter_packed(full, axis_name):
    cur = full
    for dim in ('z', 'y', 'x', 'c'):
        mine = bit_of(axis_name, dim)
        half = cur.shape[0] // 2
        low, high = cur[:half], cur[half:]
        give = jnp.where(mine == 0, high, low)
        keep = jnp.where(mine == 0, low, high)
        cur = keep + swap(give, axis_name, dim)
    return cur[0]


def pack_params(b_attn, ln_par, b_up, b_down):
    layers = b_attn.shape[0]
    flat = jnp.concatenate([b_attn.reshape(layers, -1), ln_par.reshape(layers, -1), b_up, b_down], axis=1)
    return flat


def unpack_params(full, layer, n, nu):
    part = full[:, layer].astype(jnp.float32)
    b_attn = part[:, :4 * n].reshape(16, 4, n).transpose(1, 0, 2).reshape(4, 16 * n)
    ln = part[:, 4 * n:8 * n].reshape(16, 4, n).transpose(1, 0, 2).reshape(4, 16 * n)
    b_up = part[:, 8 * n:8 * n + nu].reshape(1, 16 * nu)
    b_down = part[:, 8 * n + nu:].reshape(1, 16 * n)
    return b_attn, ln, b_up, b_down


def solution(mesh):
    axis_name = mesh.axis_names[0]
    batch_spec = P(axis_name)
    weight_specs = (P(None, None, axis_name, None), P(None, None, axis_name), P(None, None, axis_name),
                    P(None, axis_name, None), P(None, axis_name), P(None, axis_name, None), P(None, axis_name))

    def device_step(x, lengths, d_y, w_attn, b_attn, ln_par, w_up, b_up, w_down, b_down):
        layers = w_attn.shape[0]
        seqs, seq_len, width = x.shape
        tokens = seqs * seq_len
        n, nu = b_attn.shape[2], b_up.shape[1]
        cos, sin = rotary_tables()
        gather = functools.partial(lax.all_gather, axis_name=axis_name, tiled=True)
        after = lax.optimization_barrier

        def total(parts):
            return jnp.sum(parts.astype(jnp.float32), axis=0)

        small = gather_packed(pack_params(b_attn, ln_par, b_up, b_down), axis_name)
        hidden = x.reshape(tokens, width)
        saved = []
        for l in range(layers):
            ba, ln, bu, bd = unpack_params(small, l, n, nu)
            wa = gather(w_attn[l], axis=1)
            wu = gather(w_up[l], axis=0)
            wd = gather(w_down[l], axis=0)
            h_one, q, k, v = qkv(hidden, wa, ba, ln, cos, sin)
            ctx, probs = attn_fwd(lengths, q, k, v)
            mid, h_two = out_proj(ctx, hidden, wa, ba, ln)
            act, slope, out = mlp(h_two, mid, wu, bu, wd, bd)
            saved.append((hidden, h_one, q, k, v, ctx, probs, mid, h_two, act, slope, wa, wu, wd, ln))
            hidden = out
        grad = d_y.reshape(tokens, width)
        grads = [None] * layers
        number = 0
        waiting = None
        for l in reversed(range(layers)):
            x_in, h_one, q, k, v, ctx, probs, mid, h_two, act, slope, wa, wu, wd, ln = saved[l]
            pair_down, grad = after((down_grad(axis_name, number, act, grad), grad))
            carried = [pair_down] if l + 1 == layers else [waiting]
            d_pre, d_mid, d_ctx, gb_up, gln_two, landed = mlp_back(axis_name, number + 1, carried, grad, slope, wd, wu, mid, ln, wa)
            if l + 1 == layers:
                g_down, carried = total(landed), []
            else:
                grads[l + 1][0], carried = total(landed), [pair_down]
            pair_up, d_ctx = after((up_grad(axis_name, number + 2, h_two, d_pre), d_ctx))
            dq, dk, dv, landed, *rest = attn_bwd(axis_name, number + 3, [pair_up] + carried, q, k, v, ctx, d_ctx, probs, cos, sin)
            g_up = total(landed)
            if rest:
                g_down = total(rest[0])
            waiting, gb_attn = attn_grad(axis_name, number + 4, h_one, ctx, dq, dk, dv, d_mid)
            waiting, dq = after((waiting, dq))
            carried = [waiting] if l == 0 else []
            grad, gln_one, *rest = in_back(axis_name, number + 5, carried, dq, dk, dv, wa, x_in, ln, d_mid)
            g_attn = total(rest[0]) if rest else None
            number += 6
            sums_two = jnp.sum(gln_two.reshape(3, 8, width), axis=1)
            sums_one = jnp.sum(gln_one.reshape(2, 8, width), axis=1)
            gb_four = jnp.sum(gb_attn.reshape(4, 8, width), axis=1)
            gb_wide = jnp.sum(gb_up, axis=0)
            by_dev = lambda s: s.reshape(-1, 16, n).transpose(1, 0, 2).reshape(16, -1)
            packed = jnp.concatenate([by_dev(gb_four), by_dev(sums_one), by_dev(sums_two[:2]),
                                      gb_wide.reshape(16, nu), by_dev(sums_two[2:3])], axis=1)
            grads[l] = [g_attn, g_up, g_down, packed]
        got = scatter_packed(jnp.stack([g[3] for g in grads], axis=1), axis_name)
        g_attn, g_up, g_down = (jnp.stack([g[i] for g in grads]) for i in range(3))
        return (grad.reshape(x.shape), g_attn, got[:, :4 * n].reshape(layers, 4, n), got[:, 4 * n:8 * n].reshape(layers, 4, n),
                g_up, got[:, 8 * n:8 * n + nu], g_down, got[:, 8 * n + nu:])

    return jax.shard_map(device_step, mesh=mesh,
                         in_specs=(batch_spec, batch_spec, batch_spec) + weight_specs,
                         out_specs=(batch_spec,) + weight_specs,
                         check_vma=False)
```

```python
import functools, math
import jax
import jax.numpy as jnp
from jax import lax
from jax.experimental import pallas as pl
from jax.experimental.pallas import tpu as pltpu
from jax.sharding import PartitionSpec as P

HEAD_DIM = 64
SEQ = 1024
QT = 256
RB = 64
PAIR = 2 * HEAD_DIM
NEG_BIG = -1e30
NN = (((1,), (0,)), ((), ()))
NT = (((1,), (1,)), ((), ()))
TN = (((0,), (0,)), ((), ()))


def dot(a, b, dims):
    return lax.dot_general(a, b, dims, preferred_element_type=jnp.float32)


def lane_iota(rows):
    return lax.broadcasted_iota(jnp.int32, (rows, PAIR), 1)


def attn_fwd_kernel(len_ref, q_ref, k_ref, v_ref, ctx_ref, p_ref, ka_ref, qa_ref, vt_ref, e_ref, top_ref, sum_ref, ctxt_ref):
    seq_len = len_ref[pl.program_id(0)]
    lane = lane_iota(1)
    hidden_key = lax.broadcasted_iota(jnp.int32, (SEQ, PAIR), 0) >= seq_len
    for h in range(2):
        mine = (lane // HEAD_DIM) == h
        aux = lane == (1 - h) * HEAD_DIM
        own = mine.astype(jnp.float32).astype(jnp.bfloat16)
        one = aux.astype(jnp.float32).astype(jnp.bfloat16)
        bar = jnp.where(aux, NEG_BIG, 0.0).astype(jnp.bfloat16)
        ka_ref[h] = jnp.where(hidden_key, jnp.broadcast_to(bar, (SEQ, PAIR)), k_ref[...] * own)
        qa_ref[h] = q_ref[...] * own + one
    vt_ref[...] = v_ref[...].T

    def at(t):
        return pl.ds(pl.multiple_of(t * QT, QT), QT)

    def fold(x, op):
        while x.shape[0] > 8:
            half = x.shape[0] // 2
            x = op(x[:half], x[half:])
        return x

    def spread(x):
        return jnp.concatenate([x] * (RB // 8), axis=0)

    def rise(t, h):
        s = dot(ka_ref[h], qa_ref[h, at(t)], NT)
        for c in range(SEQ // RB):
            part = s[c * RB:(c + 1) * RB]
            top = fold(part, jnp.maximum)
            e = jnp.exp(part - spread(top))
            e_ref[h, c * RB:(c + 1) * RB] = e
            top_ref[h, c * 8:(c + 1) * 8] = top
            sum_ref[h, c * 8:(c + 1) * 8] = fold(e, jnp.add)

    def settle(t, h):
        tops = top_ref[h]
        weight = jnp.exp(tops - jnp.max(tops, axis=0, keepdims=True))
        scale = weight * (1.0 / jnp.sum(weight * sum_ref[h], axis=0, keepdims=True))
        for c in range(SEQ // RB):
            p_ref[h, c * RB:(c + 1) * RB, at(t)] = (e_ref[h, c * RB:(c + 1) * RB] * spread(scale[c * 8:(c + 1) * 8])).astype(jnp.bfloat16)
        rows = slice(h * HEAD_DIM, (h + 1) * HEAD_DIM)
        ctxt_ref[rows, at(t)] = dot(vt_ref[rows], p_ref[h, :, at(t)], NN)

    last = SEQ // QT - 1
    rise(0, 0)

    def turn(t, _):
        settle(t, 0)
        rise(t, 1)
        rise(jnp.minimum(t + 1, last), 0)
        settle(t, 1)
        return 0

    lax.fori_loop(0, SEQ // QT, turn, 0)
    ctx_ref[...] = ctxt_ref[...].T.astype(jnp.bfloat16)


def attn_fwd(lengths, q, k, v):
    tokens, width = q.shape
    seqs, pairs = tokens // SEQ, width // PAIR
    spec = pl.BlockSpec((SEQ, PAIR), lambda b, h, n: (b, h))
    return pl.pallas_call(
        attn_fwd_kernel,
        grid_spec=pltpu.PrefetchScalarGridSpec(
            num_scalar_prefetch=1, grid=(seqs, pairs),
            in_specs=[spec, spec, spec],
            out_specs=[spec, pl.BlockSpec((None, 2, SEQ, SEQ), lambda b, h, n: (b, h, 0, 0))],
            scratch_shapes=[pltpu.VMEM((2, SEQ, PAIR), jnp.bfloat16), pltpu.VMEM((2, SEQ, PAIR), jnp.bfloat16),
                            pltpu.VMEM((PAIR, SEQ), jnp.bfloat16), pltpu.VMEM((2, SEQ, QT), jnp.float32), pltpu.VMEM((2, SEQ // RB * 8, QT), jnp.float32), pltpu.VMEM((2, SEQ // RB * 8, QT), jnp.float32),
                            pltpu.VMEM((PAIR, SEQ), jnp.float32)]),
        out_shape=[jax.ShapeDtypeStruct((tokens, width), jnp.bfloat16),
                   jax.ShapeDtypeStruct((seqs, 2 * pairs, SEQ, SEQ), jnp.bfloat16)],
        compiler_params=pltpu.CompilerParams(dimension_semantics=("arbitrary", "arbitrary"), vmem_limit_bytes=56 << 20),
        cost_estimate=pl.CostEstimate(flops=4 * tokens * SEQ * width * 4, bytes_accessed=90 << 20, transcendentals=tokens * SEQ * 16),
        name='attn_fwd',
    )(lengths, q, k, v)


def spin(x, cos, sin, sign):
    half = HEAD_DIM // 2
    low = (lax.broadcasted_iota(jnp.int32, x.shape, 1) % HEAD_DIM) < half
    other = jnp.where(low, pltpu.roll(x, PAIR - half, 1), pltpu.roll(x, half, 1))
    return x * cos + other * (sin * sign)


def attn_bwd_kernel(axis, units, turns, q_ref, k_ref, v_ref, o_ref, do_ref, p_ref, cos_ref, sin_ref, *refs):
    pairs, (dq_ref, dk_ref, dv_ref), lands = refs[:units], refs[units:units + 3], refs[units + 3:2 * units + 3]
    doh_ref, qh_ref, kt_ref, d_ref, ds_ref, dqt_ref, *sems = refs[2 * units + 3:]
    ride(axis, pl.program_id(0) * pl.num_programs(1) + pl.program_id(1), turns, pairs, lands, by_unit(sems, units))
    lane = lane_iota(1)
    for h in range(2):
        own = ((lane // HEAD_DIM) == h).astype(jnp.float32).astype(jnp.bfloat16)
        doh_ref[h] = do_ref[...] * own
        qh_ref[h] = q_ref[...] * own
    kt_ref[...] = k_ref[...].T
    prod = (do_ref[...].astype(jnp.float32) * o_ref[...].astype(jnp.float32)).T
    for h in range(2):
        d_ref[h:h + 1] = jnp.sum(prod[h * HEAD_DIM:(h + 1) * HEAD_DIM], axis=0, keepdims=True)
    for h in range(2):
        for t in range(SEQ // QT):
            cols = slice(t * QT, (t + 1) * QT)
            dp = dot(v_ref[...], doh_ref[h, cols], NT)
            ds_ref[h, :, cols] = (p_ref[h, :, cols].astype(jnp.float32) * (dp - d_ref[h:h + 1, cols])).astype(jnp.bfloat16)
    dv_ref[...] = (dot(p_ref[0], doh_ref[0], NN) + dot(p_ref[1], doh_ref[1], NN)).astype(jnp.bfloat16)
    for h in range(2):
        dqt_ref[h * HEAD_DIM:(h + 1) * HEAD_DIM] = dot(kt_ref[h * HEAD_DIM:(h + 1) * HEAD_DIM], ds_ref[h], NN)
    dk = dot(ds_ref[0], qh_ref[0], NN) + dot(ds_ref[1], qh_ref[1], NN)
    dk_ref[...] = spin(dk, cos_ref[...], sin_ref[...], -1.0).astype(jnp.bfloat16)
    dq_ref[...] = (spin(dqt_ref[...].T, cos_ref[...], sin_ref[...], -1.0) * (HEAD_DIM ** -0.5)).astype(jnp.bfloat16)


def attn_bwd(axis, number, units, q, k, v, ctx, d_ctx, probs, cos_tab, sin_tab):
    tokens, width = q.shape
    seqs, pairs = tokens // SEQ, width // PAIR
    spec = pl.BlockSpec((SEQ, PAIR), lambda b, h: (b, h))
    table = pl.BlockSpec((SEQ, PAIR), lambda b, h: (0, 0))
    return pl.pallas_call(
        functools.partial(attn_bwd_kernel, axis, len(units), (1, 8, 12, 14) if len(units) > 1 else (1, 6, 9, 11)), grid=(seqs, pairs),
        in_specs=[spec] * 5 + [pl.BlockSpec((None, 2, SEQ, SEQ), lambda b, h: (b, h, 0, 0)), table, table] + ride_specs(units),
        out_specs=[spec] * 3 + ride_specs(units),
        scratch_shapes=[pltpu.VMEM((2, SEQ, PAIR), jnp.bfloat16), pltpu.VMEM((2, SEQ, PAIR), jnp.bfloat16),
                        pltpu.VMEM((PAIR, SEQ), jnp.bfloat16), pltpu.VMEM((8, SEQ), jnp.float32),
                        pltpu.VMEM((2, SEQ, SEQ), jnp.bfloat16), pltpu.VMEM((PAIR, SEQ), jnp.float32)] + ride_scratch(units),
        out_shape=[jax.ShapeDtypeStruct((tokens, width), jnp.bfloat16)] * 3 + sums(units),
        compiler_params=ride_params(number, 'arbitrary', 'arbitrary'),
        cost_estimate=pl.CostEstimate(flops=8 * tokens * SEQ * width * 4, bytes_accessed=100 << 20, transcendentals=0),
        name='attn_bwd',
    )(q, k, v, ctx, d_ctx, probs, cos_tab, sin_tab, *units)


EPS = 1e-5
THETA = 10000.0
HIGH = 60 << 20


def whole(shape):
    return pl.BlockSpec(shape, lambda *i: (0,) * len(shape), pipeline_mode=pl.Buffered(1))


def part_of(shape, *at):
    return pl.BlockSpec(shape, lambda *i: at, pipeline_mode=pl.Buffered(1))


def partial(shape):
    return pl.BlockSpec(shape, lambda *i: (0,) * len(shape))


def rows_of(block, width):
    return pl.BlockSpec((block, width), lambda i: (i, 0))


def params(*semantics):
    return pltpu.CompilerParams(dimension_semantics=semantics or ('arbitrary',), vmem_limit_bytes=HIGH)


def cost(flops, moved):
    return pl.CostEstimate(flops=flops, bytes_accessed=moved, transcendentals=0)


def normal(x):
    mean = jnp.mean(x, axis=-1, keepdims=True)
    centered = x - mean
    inv = lax.rsqrt(jnp.mean(centered * centered, axis=-1, keepdims=True) + EPS)
    return centered * inv, inv


def norm_back(x, gain, grad):
    unit, inv = normal(x)
    scaled = grad * gain
    inner = scaled - jnp.mean(scaled, axis=-1, keepdims=True) - unit * jnp.mean(scaled * unit, axis=-1, keepdims=True)
    return inv * inner, unit


def eights(x):
    return jnp.sum(x.reshape(x.shape[0] // 8, 8, x.shape[1]), axis=0)


ORDERS = ((1, 2, 4), (2, 4, 1), (4, 1, 2))


def thirds(width):
    tiles = width // 128
    cuts = [0, (tiles + 2) // 3, (2 * tiles + 2) // 3, tiles]
    return [(128 * lo, 128 * hi) for lo, hi in zip(cuts, cuts[1:])]


def ride(axis, step, turns, pair_refs, sum_refs, scratch):
    me = lax.axis_index(axis)
    side, chip = me % 2, me // 2
    units = len(pair_refs)

    def bit(weight):
        return (chip // weight) % 2

    def beside(weight):
        return (chip + weight - 2 * weight * bit(weight)) * 2 + side

    def send(u, o, j, source, target, weight):
        sems = scratch[u][-2:]
        return pltpu.make_async_remote_copy(
            src_ref=source, dst_ref=target, send_sem=sems[0].at[o, j], recv_sem=sems[1].at[o, j],
            device_id=(beside(weight),), device_id_type=MESH)

    def lanes(u, o):
        lo, hi = thirds(pair_refs[u].shape[2])[o]
        return slice(lo, hi)

    def fetch(u):
        return pltpu.make_async_copy(pair_refs[u], scratch[u][0], scratch[u][-3].at[0])

    def store(u):
        return pltpu.make_async_copy(scratch[u][7], sum_refs[u], scratch[u][-3].at[0])

    def first(u, o):
        mine, in_one = scratch[u][0], scratch[u][1]
        w, cols = ORDERS[o], lanes(u, o)
        return [send(u, o, 2 * i + j, mine.at[(1 - bit(w[0])) * w[0] + i * w[1] + j * w[2], :, cols], in_one.at[2 * i + j, :, cols], w[0])
                for i in range(2) for j in range(2)]

    def second(u, o):
        w, cols = ORDERS[o], lanes(u, o)
        return [send(u, o, 4 + j, scratch[u][5].at[j, :, cols], scratch[u][2].at[j, :, cols], w[1]) for j in range(2)]

    def third(u, o):
        w, cols = ORDERS[o], lanes(u, o)
        return [send(u, o, 6, scratch[u][6].at[:, cols], scratch[u][3].at[:, cols], w[2])]

    each = [(u, o) for u in range(units) for o in range(3)]

    @pl.when(step == 0)
    def _():
        for u in range(units):
            fetch(u).start()
        barrier = pltpu.get_barrier_semaphore()
        for w in ORDERS[0]:
            pl.semaphore_signal(barrier, inc=1, device_id=(beside(w),), device_id_type=MESH)

    @pl.when(step == turns[0])
    def _():
        for u in range(units):
            fetch(u).wait()
        pl.semaphore_wait(pltpu.get_barrier_semaphore(), 3)
        for u, o in each:
            for c in first(u, o):
                c.start()

    @pl.when(step == turns[1])
    def _():
        for u, o in each:
            mine, in_one, _, _, kept, out_two = scratch[u][:6]
            w, cols = ORDERS[o], lanes(u, o)
            for c in first(u, o):
                c.wait()
            stay = bit(w[1])
            for j in range(2):
                base = bit(w[0]) * w[0] + j * w[2]
                kept[j, :, cols] = mine[base + stay * w[1], :, cols].astype(jnp.float32) + in_one[2 * stay + j, :, cols].astype(jnp.float32)
                out_two[j, :, cols] = (mine[base + (1 - stay) * w[1], :, cols].astype(jnp.float32)
                                       + in_one[2 * (1 - stay) + j, :, cols].astype(jnp.float32)).astype(jnp.bfloat16)
            for c in second(u, o):
                c.start()

    @pl.when(step == turns[2])
    def _():
        for u, o in each:
            _, _, in_two, _, kept, _, out_three, final = scratch[u][:8]
            w, cols = ORDERS[o], lanes(u, o)
            for c in second(u, o):
                c.wait()
            stay = bit(w[2])
            final[:, cols] = kept[stay, :, cols] + in_two[stay, :, cols].astype(jnp.float32)
            out_three[:, cols] = (kept[1 - stay, :, cols] + in_two[1 - stay, :, cols].astype(jnp.float32)).astype(jnp.bfloat16)
            for c in third(u, o):
                c.start()

    @pl.when(step == turns[3])
    def _():
        for u, o in each:
            in_three, final = scratch[u][3], scratch[u][7]
            cols = lanes(u, o)
            for c in third(u, o):
                c.wait()
            final[:, cols] += in_three[:, cols].astype(jnp.float32)
        for u in range(units):
            store(u).start()
        for u in range(units):
            store(u).wait()


MESH = pl.DeviceIdType.MESH


def ride_scratch(pairs):
    made = []
    for p in pairs:
        chips, rows, width = p.shape
        half = lambda *lead: pltpu.VMEM(lead + (rows, width), jnp.bfloat16)
        full = lambda *lead: pltpu.VMEM(lead + (rows, width), jnp.float32)
        made += [half(chips), half(4), half(2), half(), full(2), half(2), half(), full(),
                 pltpu.SemaphoreType.DMA((1,)), pltpu.SemaphoreType.DMA((3, 7)), pltpu.SemaphoreType.DMA((3, 7))]
    return made


def by_unit(refs, units):
    return [refs[11 * u:11 * u + 11] for u in range(units)]


def ride_specs(pairs):
    return [pl.BlockSpec(memory_space=pl.ANY)] * len(pairs)


def sums(pairs):
    return [jax.ShapeDtypeStruct(p.shape[1:], jnp.float32) for p in pairs]


def ride_params(number, *semantics):
    return pltpu.CompilerParams(dimension_semantics=semantics or ('arbitrary',), vmem_limit_bytes=HIGH, collective_id=number, has_side_effects=True)


def qkv_kernel(x_ref, w_ref, b_ref, ln_ref, cos_ref, sin_ref, h_ref, q_ref, k_ref, v_ref):
    unit, _ = normal(x_ref[...].astype(jnp.float32))
    h_ref[...] = (unit * ln_ref[0:1] + ln_ref[1:2]).astype(jnp.bfloat16)
    for j, out_ref in enumerate((q_ref, k_ref, v_ref)):
        full = dot(h_ref[...], w_ref[j], NN) + b_ref[j:j + 1]
        if j == 2:
            out_ref[...] = full.astype(jnp.bfloat16)
            continue
        if j == 0:
            full = full * (HEAD_DIM ** -0.5)
        for c in range(0, full.shape[1], PAIR):
            out_ref[:, c:c + PAIR] = spin(full[:, c:c + PAIR], cos_ref[...], sin_ref[...], 1.0).astype(jnp.bfloat16)


def qkv(x, w, b, ln, cos, sin):
    tokens, width = x.shape
    block = 512
    row = rows_of(block, width)
    table = pl.BlockSpec((block, PAIR), lambda i: (i % (SEQ // block), 0))
    return pl.pallas_call(
        qkv_kernel, grid=(tokens // block,),
        in_specs=[row, part_of((3, width, width), 0, 0, 0), whole(b.shape), whole(ln.shape), table, table],
        out_specs=[row] * 4,
        out_shape=[jax.ShapeDtypeStruct(x.shape, jnp.bfloat16)] * 4,
        compiler_params=params(), cost_estimate=cost(6 * tokens * width * width, 26 << 20), name='qkv',
    )(x, w, b, ln, cos, sin)


def out_kernel(ctx_ref, x_ref, w_ref, b_ref, ln_ref, mid_ref, h_ref):
    mid = (x_ref[...].astype(jnp.float32) + dot(ctx_ref[...], w_ref[...], NN) + b_ref[3:4]).astype(jnp.bfloat16)
    mid_ref[...] = mid
    unit, _ = normal(mid.astype(jnp.float32))
    h_ref[...] = (unit * ln_ref[2:3] + ln_ref[3:4]).astype(jnp.bfloat16)


def out_proj(ctx, x, w, b, ln):
    tokens, width = x.shape
    block = 512
    row = rows_of(block, width)
    return pl.pallas_call(
        out_kernel, grid=(tokens // block,),
        in_specs=[row, row, part_of((None, width, width), 3, 0, 0), whole(b.shape), whole(ln.shape)], out_specs=[row] * 2,
        out_shape=[jax.ShapeDtypeStruct(x.shape, jnp.bfloat16)] * 2,
        compiler_params=params(), cost_estimate=cost(2 * tokens * width * width, 18 << 20), name='out_proj',
    )(ctx, x, w, b, ln)


def mlp_kernel(h_ref, mid_ref, wu_ref, bu_ref, wd_ref, bd_ref, act_ref, slope_ref, y_ref):
    total = mid_ref[...].astype(jnp.float32) + bd_ref[...]
    wide = wu_ref.shape[1]
    for c in range(0, wide, 1024):
        cols = slice(c, c + 1024)
        pre = dot(h_ref[...], wu_ref[:, cols], NN) + bu_ref[:, cols]
        cdf = 0.5 + 0.5 * lax.erf(pre * (1.0 / math.sqrt(2.0)))
        act_ref[:, cols] = (pre * cdf).astype(jnp.bfloat16)
        slope_ref[:, cols] = cdf + pre * (jnp.exp(-0.5 * pre * pre) * (1.0 / math.sqrt(2.0 * math.pi)))
        total = total + dot(act_ref[:, cols], wd_ref[cols], NN)
    y_ref[...] = total.astype(jnp.bfloat16)


def mlp(h, mid, wu, bu, wd, bd):
    tokens, width = h.shape
    wide = wu.shape[1]
    block = 256
    row, long = rows_of(block, width), rows_of(block, wide)
    return pl.pallas_call(
        mlp_kernel, grid=(tokens // block,),
        in_specs=[row, row, whole(wu.shape), whole(bu.shape), whole(wd.shape), whole(bd.shape)],
        out_specs=[long, long, row],
        out_shape=[jax.ShapeDtypeStruct((tokens, wide), jnp.bfloat16), jax.ShapeDtypeStruct((tokens, wide), jnp.float32),
                   jax.ShapeDtypeStruct(h.shape, jnp.bfloat16)],
        compiler_params=params(), cost_estimate=cost(4 * tokens * width * wide, 80 << 20), name='mlp',
    )(h, mid, wu, bu, wd, bd)


def mlp_back_kernel(axis, units, turns, dy_ref, slope_ref, wd_ref, wu_ref, mid_ref, ln_ref, wo_ref, *refs):
    pairs, (dpre_ref, dmid_ref, dctx_ref, gbu_ref, gln_ref), lands, sems = refs[:units], refs[units:units + 5], refs[units + 5:2 * units + 5], refs[2 * units + 5:]
    ride(axis, pl.program_id(0), turns, pairs, lands, by_unit(sems, units))
    dy = dy_ref[...]
    grad = None
    wide = wu_ref.shape[1]
    first = pl.program_id(0) == 0

    @pl.when(first)
    def _():
        gbu_ref[...] = jnp.zeros_like(gbu_ref)
        gln_ref[...] = jnp.zeros_like(gln_ref)

    for c in range(0, wide, 1024):
        cols = slice(c, c + 1024)
        dpre = dot(dy, wd_ref[cols], NT) * slope_ref[:, cols]
        gbu_ref[:, cols] += eights(dpre)
        dpre_ref[:, cols] = dpre.astype(jnp.bfloat16)
        part = dot(dpre_ref[:, cols], wu_ref[:, cols], NT)
        grad = part if grad is None else grad + part
    dy = dy.astype(jnp.float32)
    back, unit = norm_back(mid_ref[...].astype(jnp.float32), ln_ref[2:3], grad)
    dmid = (dy + back).astype(jnp.bfloat16)
    dmid_ref[...] = dmid
    gln_ref[0:8] += eights(grad * unit)
    gln_ref[8:16] += eights(grad)
    gln_ref[16:24] += eights(dy)
    dctx_ref[...] = dot(dmid, wo_ref[...], NT).astype(jnp.bfloat16)


def mlp_back(axis, number, pairs, dy, slope, wd, wu, mid, ln, wo):
    tokens, width = dy.shape
    wide = wu.shape[1]
    block = 256
    row, long = rows_of(block, width), rows_of(block, wide)
    half = jax.ShapeDtypeStruct(dy.shape, jnp.bfloat16)
    return pl.pallas_call(
        functools.partial(mlp_back_kernel, axis, len(pairs), (1, 4, 6, 7)), grid=(tokens // block,),
        in_specs=[row, long, whole(wd.shape), whole(wu.shape), row, whole(ln.shape), part_of((None, width, width), 3, 0, 0)] + ride_specs(pairs),
        out_specs=[long, row, row, partial((8, wide)), partial((24, width))] + ride_specs(pairs),
        out_shape=[jax.ShapeDtypeStruct((tokens, wide), jnp.bfloat16), half, half,
                   jax.ShapeDtypeStruct((8, wide), jnp.float32), jax.ShapeDtypeStruct((24, width), jnp.float32)] + sums(pairs),
        scratch_shapes=ride_scratch(pairs),
        compiler_params=ride_params(number), cost_estimate=cost(2 * tokens * width * (2 * wide + width), 90 << 20), name='mlp_back',
    )(dy, slope, wd, wu, mid, ln, wo, *pairs)


def in_back_kernel(axis, units, turns, dq_ref, dk_ref, dv_ref, w_ref, x_ref, ln_ref, dmid_ref, *refs):
    pairs, (dx_ref, gln_ref), lands, sems = refs[:units], refs[units:units + 2], refs[units + 2:2 * units + 2], refs[2 * units + 2:]
    if units:
        ride(axis, pl.program_id(0), turns, pairs, lands, by_unit(sems, units))

    @pl.when(pl.program_id(0) == 0)
    def _():
        gln_ref[...] = jnp.zeros_like(gln_ref)

    grad = dot(dq_ref[...], w_ref[0], NT) + dot(dk_ref[...], w_ref[1], NT) + dot(dv_ref[...], w_ref[2], NT)
    back, unit = norm_back(x_ref[...].astype(jnp.float32), ln_ref[0:1], grad)
    dx_ref[...] = (dmid_ref[...].astype(jnp.float32) + back).astype(jnp.bfloat16)
    gln_ref[0:8] += eights(grad * unit)
    gln_ref[8:16] += eights(grad)


def in_back(axis, number, pairs, dq, dk, dv, w, x, ln, dmid):
    tokens, width = x.shape
    block = 256
    row = rows_of(block, width)
    return pl.pallas_call(
        functools.partial(in_back_kernel, axis, len(pairs), (1, 6, 7, 7)), grid=(tokens // block,),
        in_specs=[row, row, row, part_of((3, width, width), 0, 0, 0), row, whole(ln.shape), row] + ride_specs(pairs),
        out_specs=[row, partial((16, width))] + ride_specs(pairs),
        out_shape=[jax.ShapeDtypeStruct(x.shape, jnp.bfloat16), jax.ShapeDtypeStruct((16, width), jnp.float32)] + sums(pairs),
        scratch_shapes=ride_scratch(pairs) if pairs else [],
        compiler_params=ride_params(number) if pairs else params(), cost_estimate=cost(6 * tokens * width * width, 34 << 20), name='in_back',
    )(dq, dk, dv, w, x, ln, dmid, *pairs)


def swap_step(axis, steps, make, keep_ref, send_ref, recv_ref, send_sem, recv_sem, out_ref):
    i = pl.program_id(0)
    me = lax.axis_index(axis)
    side = me % 2
    other = me + 1 - 2 * side

    def copy(j):
        return pltpu.make_async_remote_copy(
            src_ref=send_ref.at[j], dst_ref=recv_ref.at[j], send_sem=send_sem.at[j], recv_sem=recv_sem.at[j],
            device_id=(other,), device_id_type=MESH)

    def put(at, low, high):
        keep_ref[(i % 3,) + at] = jnp.where(side == 0, low, high)
        send_ref[(i,) + at] = jnp.where(side == 0, high, low).astype(jnp.bfloat16)

    def finish():
        out_ref[...] = (keep_ref[(i + 1) % 3] + recv_ref[i - 2].astype(jnp.float32)).astype(jnp.bfloat16)

    @pl.when(i == 0)
    def _():
        barrier = pltpu.get_barrier_semaphore()
        pl.semaphore_signal(barrier, inc=1, device_id=(other,), device_id_type=MESH)
        pl.semaphore_wait(barrier, 1)

    @pl.when((i >= 1) & (i <= steps))
    def _():
        copy(i - 1).start()

    @pl.when(i >= 2)
    def _():
        copy(i - 2).wait()

    @pl.when(i < 2)
    def _():
        make(put)

    @pl.when((i >= 2) & (i < steps))
    def _():
        make(put)
        finish()

    @pl.when(i >= steps)
    def _():
        finish()


def swap_scratch(steps, block):
    return [pltpu.VMEM((3,) + block, jnp.float32), pltpu.VMEM((steps,) + block, jnp.bfloat16), pltpu.VMEM((steps,) + block, jnp.bfloat16),
            pltpu.SemaphoreType.DMA((steps,)), pltpu.SemaphoreType.DMA((steps,))]


def swap_params(number):
    return pltpu.CompilerParams(dimension_semantics=('arbitrary',), vmem_limit_bytes=HIGH, collective_id=number, has_side_effects=True)


def down_grad_kernel(axis, steps, a_ref, b_ref, out_ref, *scratch):
    def make(put):
        grad = dot(a_ref[...], b_ref[...], TN)
        half = grad.shape[0] // 2
        put((), grad[:half], grad[half:])

    swap_step(axis, steps, make, *scratch, out_ref)


def down_grad(axis, number, a, b):
    tokens, m = a.shape
    n = b.shape[1]
    chips = 8
    block = m // chips
    return pl.pallas_call(
        functools.partial(down_grad_kernel, axis, chips), grid=(chips + 2,),
        in_specs=[pl.BlockSpec((tokens, block), lambda i: (0, jnp.minimum(i, chips - 1))), whole(b.shape)],
        out_specs=pl.BlockSpec((None, block // 2, n), lambda i: (jnp.maximum(i - 2, 0), 0, 0)),
        out_shape=jax.ShapeDtypeStruct((chips, block // 2, n), jnp.bfloat16),
        scratch_shapes=swap_scratch(chips, (block // 2, n)),
        compiler_params=swap_params(number), cost_estimate=cost(2 * tokens * m * n, 2 * (tokens * (m + n) + m * n)), name='down_grad',
    )(a, b)


def up_grad_kernel(axis, steps, a_ref, b_ref, out_ref, *scratch):
    def make(put):
        grad = dot(a_ref[...], b_ref[...], TN)
        chips, half = out_ref.shape[0], out_ref.shape[1]
        for c in range(chips):
            r = 2 * c * half
            put((c,), grad[r:r + half], grad[r + half:r + 2 * half])

    swap_step(axis, steps, make, *scratch, out_ref)


def up_grad(axis, number, a, b):
    tokens, m = a.shape
    n = b.shape[1]
    chips, block = 8, 512
    steps = n // block
    half = m // chips // 2
    return pl.pallas_call(
        functools.partial(up_grad_kernel, axis, steps), grid=(steps + 2,),
        in_specs=[whole(a.shape), pl.BlockSpec((tokens, block), lambda i: (0, jnp.minimum(i, steps - 1)))],
        out_specs=pl.BlockSpec((chips, half, block), lambda i: (0, 0, jnp.maximum(i - 2, 0))),
        out_shape=jax.ShapeDtypeStruct((chips, half, n), jnp.bfloat16),
        scratch_shapes=swap_scratch(steps, (chips, half, block)),
        compiler_params=swap_params(number), cost_estimate=cost(2 * tokens * m * n, 2 * (tokens * (m + n) + m * n)), name='up_grad',
    )(a, b)


def attn_grad_kernel(axis, steps, h_ref, ctx_ref, dq_ref, dk_ref, dv_ref, dmid_ref, out_ref, gb_ref, *scratch):
    def make(put):
        chips, half = out_ref.shape[0], out_ref.shape[1] // 4
        for j, d_ref in enumerate((dq_ref, dk_ref, dv_ref, dmid_ref)):
            grad = dot((h_ref if j < 3 else ctx_ref)[...], d_ref[...], TN)
            for c in range(chips):
                r = 2 * c * half
                put((c, slice(j * half, (j + 1) * half)), grad[r:r + half], grad[r + half:r + 2 * half])
            gb_ref[8 * j:8 * j + 8] = eights(d_ref[...].astype(jnp.float32))

    swap_step(axis, steps, make, *scratch, out_ref)


def attn_grad(axis, number, h, ctx, dq, dk, dv, dmid):
    tokens, width = h.shape
    chips, block = 8, 256
    steps = width // block
    half = width // chips // 2
    cols = pl.BlockSpec((tokens, block), lambda i: (0, jnp.minimum(i, steps - 1)))
    return pl.pallas_call(
        functools.partial(attn_grad_kernel, axis, steps), grid=(steps + 2,),
        in_specs=[whole(h.shape), whole(ctx.shape), cols, cols, cols, cols],
        out_specs=[pl.BlockSpec((chips, 4 * half, block), lambda i: (0, 0, jnp.maximum(i - 2, 0))),
                   pl.BlockSpec((32, block), lambda i: (0, jnp.minimum(i, steps - 1)))],
        out_shape=[jax.ShapeDtypeStruct((chips, 4 * half, width), jnp.bfloat16), jax.ShapeDtypeStruct((32, width), jnp.float32)],
        scratch_shapes=swap_scratch(steps, (chips, 4 * half, block)),
        compiler_params=swap_params(number), cost_estimate=cost(8 * tokens * width * width, 32 << 20), name='attn_grad',
    )(h, ctx, dq, dk, dv, dmid)


def small_kernel(axis, in_ref, out_ref, land_ref, send_sem, recv_sem):
    me = lax.axis_index(axis)
    count = in_ref.shape[0]
    barrier = pltpu.get_barrier_semaphore()
    for j in range(1, count):
        pl.semaphore_signal(barrier, inc=1, device_id=((me + j) % count,), device_id_type=MESH)
    pl.semaphore_wait(barrier, count - 1)
    copies = [pltpu.make_async_remote_copy(
        src_ref=in_ref.at[(me + j) % count], dst_ref=land_ref.at[j], send_sem=send_sem.at[j], recv_sem=recv_sem.at[j],
        device_id=((me + j) % count,), device_id_type=MESH) for j in range(1, count)]
    for c in copies:
        c.start()
    total = in_ref[me]
    for c in copies:
        c.wait()
    for j in range(1, count):
        total = total + land_ref[j]
    out_ref[...] = total


def small_sums(axis, number, packed):
    count = packed.shape[0]
    return pl.pallas_call(
        functools.partial(small_kernel, axis),
        in_specs=[pl.BlockSpec(memory_space=pltpu.VMEM)], out_specs=pl.BlockSpec(memory_space=pltpu.VMEM),
        out_shape=jax.ShapeDtypeStruct(packed.shape[1:], jnp.float32),
        scratch_shapes=[pltpu.VMEM(packed.shape, jnp.float32), pltpu.SemaphoreType.DMA((count,)), pltpu.SemaphoreType.DMA((count,))],
        compiler_params=pltpu.CompilerParams(collective_id=number, has_side_effects=True), name='small_sums',
    )(packed)


def rotary_tables():
    half = HEAD_DIM // 2
    inv_freq = 1.0 / (THETA ** (jnp.arange(half, dtype=jnp.float32) * (2.0 / HEAD_DIM)))
    angles = jnp.arange(SEQ, dtype=jnp.float32)[:, None] * inv_freq[None, :]
    cos, sin = jnp.cos(angles), jnp.sin(angles)
    return jnp.concatenate([cos] * 4, axis=1), jnp.concatenate([-sin, sin, -sin, sin], axis=1)


BITS = {'c': 1, 'x': 2, 'y': 4, 'z': 8}


def swap(value, axis_name, dim):
    return lax.ppermute(value, axis_name, [(i, i ^ BITS[dim]) for i in range(16)])


def bit_of(axis_name, dim):
    return (lax.axis_index(axis_name) // BITS[dim]) % 2


def gather_packed(packed, axis_name):
    held = packed[None]
    for dim in ('c', 'x', 'y', 'z'):
        got = swap(held, axis_name, dim)
        mine = bit_of(axis_name, dim)
        held = jnp.where(mine == 0, jnp.concatenate([held, got]), jnp.concatenate([got, held]))
    return held


def pack_params(b_attn, ln_par, b_up, b_down):
    layers = b_attn.shape[0]
    flat = jnp.concatenate([b_attn.reshape(layers, -1), ln_par.reshape(layers, -1), b_up, b_down], axis=1)
    return flat


def unpack_params(full, layer, n, nu):
    part = full[:, layer].astype(jnp.float32)
    b_attn = part[:, :4 * n].reshape(16, 4, n).transpose(1, 0, 2).reshape(4, 16 * n)
    ln = part[:, 4 * n:8 * n].reshape(16, 4, n).transpose(1, 0, 2).reshape(4, 16 * n)
    b_up = part[:, 8 * n:8 * n + nu].reshape(1, 16 * nu)
    b_down = part[:, 8 * n + nu:].reshape(1, 16 * n)
    return b_attn, ln, b_up, b_down


def solution(mesh):
    axis_name = mesh.axis_names[0]
    batch_spec = P(axis_name)
    weight_specs = (P(None, None, axis_name, None), P(None, None, axis_name), P(None, None, axis_name),
                    P(None, axis_name, None), P(None, axis_name), P(None, axis_name, None), P(None, axis_name))

    def device_step(x, lengths, d_y, w_attn, b_attn, ln_par, w_up, b_up, w_down, b_down):
        layers = w_attn.shape[0]
        seqs, seq_len, width = x.shape
        tokens = seqs * seq_len
        n, nu = b_attn.shape[2], b_up.shape[1]
        cos, sin = rotary_tables()
        gather = functools.partial(lax.all_gather, axis_name=axis_name, tiled=True)
        after = lax.optimization_barrier

        small = gather_packed(pack_params(b_attn, ln_par, b_up, b_down), axis_name)
        hidden = x.reshape(tokens, width)
        saved = []
        for l in range(layers):
            ba, ln, bu, bd = unpack_params(small, l, n, nu)
            wa = gather(w_attn[l], axis=1)
            wu = gather(w_up[l], axis=0)
            wd = gather(w_down[l], axis=0)
            h_one, q, k, v = qkv(hidden, wa, ba, ln, cos, sin)
            ctx, probs = attn_fwd(lengths, q, k, v)
            mid, h_two = out_proj(ctx, hidden, wa, ba, ln)
            act, slope, out = mlp(h_two, mid, wu, bu, wd, bd)
            saved.append((hidden, h_one, q, k, v, ctx, probs, mid, h_two, act, slope, wa, wu, wd, ln))
            hidden = out
        grad = d_y.reshape(tokens, width)
        grads = [None] * layers
        number = 0
        waiting = None
        for l in reversed(range(layers)):
            x_in, h_one, q, k, v, ctx, probs, mid, h_two, act, slope, wa, wu, wd, ln = saved[l]
            pair_down, grad = after((down_grad(axis_name, number, act, grad), grad))
            carried = [pair_down] if l + 1 == layers else [waiting]
            d_pre, d_mid, d_ctx, gb_up, gln_two, landed = mlp_back(axis_name, number + 1, carried, grad, slope, wd, wu, mid, ln, wa)
            if l + 1 == layers:
                g_down, carried = landed, []
            else:
                grads[l + 1][0], carried = landed, [pair_down]
            pair_up, d_ctx = after((up_grad(axis_name, number + 2, h_two, d_pre), d_ctx))
            dq, dk, dv, landed, *rest = attn_bwd(axis_name, number + 3, [pair_up] + carried, q, k, v, ctx, d_ctx, probs, cos, sin)
            g_up = landed
            if rest:
                g_down = rest[0]
            waiting, gb_attn = attn_grad(axis_name, number + 4, h_one, ctx, dq, dk, dv, d_mid)
            waiting, dq = after((waiting, dq))
            carried = [waiting] if l == 0 else []
            grad, gln_one, *rest = in_back(axis_name, number + 5, carried, dq, dk, dv, wa, x_in, ln, d_mid)
            g_attn = rest[0] if rest else None
            number += 6
            sums_two = jnp.sum(gln_two.reshape(3, 8, width), axis=1)
            sums_one = jnp.sum(gln_one.reshape(2, 8, width), axis=1)
            gb_four = jnp.sum(gb_attn.reshape(4, 8, width), axis=1)
            gb_wide = jnp.sum(gb_up, axis=0)
            by_dev = lambda s: s.reshape(-1, 16, n).transpose(1, 0, 2).reshape(16, -1)
            packed = jnp.concatenate([by_dev(gb_four), by_dev(sums_one), by_dev(sums_two[:2]),
                                      gb_wide.reshape(16, nu), by_dev(sums_two[2:3])], axis=1)
            grads[l] = [g_attn, g_up, g_down, packed]
        got = small_sums(axis_name, number, jnp.stack([jnp.pad(g[3], ((0, 0), (0, 64))) for g in grads], axis=1))[:, :832]
        for g in grads:
            g[0] = g[0].reshape(4, -1, width)
        g_attn, g_up, g_down = (jnp.stack([g[i] for g in grads]) for i in range(3))
        return (grad.reshape(x.shape), g_attn, got[:, :4 * n].reshape(layers, 4, n), got[:, 4 * n:8 * n].reshape(layers, 4, n),
                g_up, got[:, 8 * n:8 * n + nu], g_down, got[:, 8 * n + nu:])

    return jax.shard_map(device_step, mesh=mesh,
                         in_specs=(batch_spec, batch_spec, batch_spec) + weight_specs,
                         out_specs=(batch_spec,) + weight_specs,
                         check_vma=False)
```
